256 devices in a mesh: ty: 8 (over z_lo, core), tx: 32 (over x, y, z_hi).
Axes of the slice: x: 4, y: 4, z: 8 (z_hi: 2, z_lo: 4; z = z_hi * 4 + z_lo), core: 2. Of those that a mesh axis runs over, the one named last changes fastest.
Arguments:
- movie: bfloat16 [256, 1024, 128], P('ty', 'tx'), may hold values from 0 to 2
- footprints: bfloat16 [8, 32, 32, 1024], P('ty', 'tx'), may hold values from 0.049804688 to 1
- centres: int32 [8, 32, 32, 2], P('ty', 'tx'), may hold values from 0 to 31
- traces: bfloat16 [8, 32, 32, 128], P('ty', 'tx'), may hold values from 0 to 1
- counts: int32 [8, 32], P('ty', 'tx'), may hold values from 8 to 32
- order: int32 [8, 32, 32], P('ty', 'tx'), may hold values from 0 to 31, each once within a row
Outputs:
- new_traces: float32 [8, 32, 32, 128], P('ty', 'tx')
The draws below stay inside these ranges and needn't reach their ends.
Inputs may be any that keep to these rules, and one draw needn't show every extreme that they name: Slots 0 to counts - 1 of a tile hold neurons; the footprints, centres and traces of the other slots are not used. order[a, b] holds each of 0 to 31 once. `centres`: A centre lies inside its owner tile.
All inputs are finite; a program needn't handle non-finite values.
Results may differ from the reference program's by a relative error of at most 0.0003.
Values may be sent and summed in bfloat16 or wider, within the bound.
A program may use at most 64 MiB of HBM per device.

```python
import jax
import jax.numpy as jnp
from jax import lax

TILE = 32
FRAMES = 128
K_DEV = 32
BLOCKS = 4
PATCH = 32
HEIGHT = 256
WIDTH = 1024
N_TY = 8
N_TX = 32


def with_ends(drawn, stream_key, least, high):
    longest = drawn.shape.index(max(drawn.shape))
    spots = []
    for shift in (0, 1):
        where = [jax.random.randint(jax.random.fold_in(stream_key, axis), (), 0, length) for axis, length in enumerate(drawn.shape)]
        where[longest] = (where[longest] + shift) % drawn.shape[longest]
        spots.append(tuple(where))
    return drawn.at[spots[0]].set(least).at[spots[1]].set(high)


def block_scale(rng, shape, split, least, high):
    def one(position, shards_of):
        heights = jax.random.uniform(jax.random.fold_in(jax.random.fold_in(rng, 6), position), (shards_of,), jnp.float32, least / len(split), high / len(split))
        return jnp.repeat(jnp.exp(heights), shape[position] // shards_of).reshape((-1,) + (1,) * (len(shape) - position - 1))

    level = one(*split[0])
    for cut in split[1:]:
        level = level * one(*cut)
    return level


def setup_inputs(seed: int = 0) -> dict:
    splits = jax.random.split(jax.random.key(seed), 7)
    movie = jnp.clip(2.0 * jax.random.uniform(splits[0], (HEIGHT, WIDTH, FRAMES), jnp.float32) ** block_scale(splits[0], (HEIGHT, WIDTH, FRAMES), ((0, 8), (1, 32)), -0.2, 0.2), 0.0, 2.0).astype(jnp.bfloat16)
    footprints = jnp.clip(0.049804688 + 0.9501953 * jax.random.uniform(splits[1], (N_TY, N_TX, K_DEV, PATCH * PATCH), jnp.float32) ** block_scale(splits[1], (N_TY, N_TX, K_DEV, PATCH * PATCH), ((0, 8), (1, 32)), -0.2, 0.2), 0.049804688, 1.0).astype(jnp.bfloat16)
    centres = with_ends(jax.random.randint(splits[2], (N_TY, N_TX, K_DEV, 2), 0, TILE), jax.random.fold_in(splits[2], 1), 0, TILE - 1).astype(jnp.int32)
    traces = jnp.clip(1.0 * jax.random.uniform(splits[3], (N_TY, N_TX, K_DEV, FRAMES), jnp.float32) ** block_scale(splits[3], (N_TY, N_TX, K_DEV, FRAMES), ((0, 8), (1, 32)), -0.2, 0.2), 0.0, 1.0).astype(jnp.bfloat16)
    counts = with_ends(jax.random.randint(splits[4], (N_TY, N_TX), K_DEV // 4, K_DEV + 1), jax.random.fold_in(splits[4], 1), K_DEV // 4, K_DEV).astype(jnp.int32)
    order = jax.vmap(lambda own: jax.random.permutation(own, K_DEV))(jax.random.split(splits[5], N_TY * N_TX)).reshape((N_TY, N_TX, K_DEV)).astype(jnp.int32)
    return {"movie": movie, "footprints": footprints, "centres": centres, "traces": traces, "counts": counts, "order": order}


precise = lax.Precision.HIGHEST


def neighbours(values):
    rows_count = values.shape[0]
    cols_count = values.shape[1]
    widths = [(1, 1), (1, 1)] + [(0, 0)] * (values.ndim - 2)
    padded = jnp.pad(values, widths)
    pieces = [padded[step_down:step_down + rows_count, step_right:step_right + cols_count] for step_down in range(3) for step_right in range(3)]
    return jnp.stack(pieces, axis=2)


def by_order(values, ordering):
    index = ordering.reshape(ordering.shape + (1,) * (values.ndim - 3))
    return jnp.take_along_axis(values, index, axis=2)


def margin_rows(own_patch, own_rows, own_cols, source_patch, source_rows, source_cols):
    widened = jnp.pad(source_patch, ((0, 0), (PATCH, PATCH), (PATCH, PATCH)))

    def window_at(source_piece, source_row, source_col, row_at, col_at):
        first_row = jnp.clip(PATCH + row_at - source_row, 0, 2 * PATCH)
        first_col = jnp.clip(PATCH + col_at - source_col, 0, 2 * PATCH)
        return lax.dynamic_slice(source_piece, (first_row, first_col), (PATCH, PATCH))

    def against(row_at, col_at):
        return jax.vmap(window_at, in_axes=(0, 0, 0, None, None))(widened, source_rows, source_cols, row_at, col_at)

    windows = jax.vmap(against)(own_rows, own_cols)
    return jnp.einsum('kij,klij->kl', own_patch.astype(jnp.float32), windows.astype(jnp.float32), precision=precise)


def reference(movie, footprints, centres, traces, counts, order):
    tiles_down = counts.shape[0]
    tiles_across = counts.shape[1]
    slot_count = footprints.shape[2]
    tile_side = movie.shape[0] // tiles_down
    frame_count = movie.shape[2]
    half_patch = PATCH // 2
    block_rows = slot_count // BLOCKS
    alive_mask = order < counts[:, :, None]
    keep_mask = alive_mask.astype(jnp.bfloat16)
    patches = by_order(footprints, order) * keep_mask[..., None]
    patches = patches.reshape(tiles_down, tiles_across, slot_count, PATCH, PATCH)
    positions = by_order(centres, order)
    row_pos = positions[..., 0]
    col_pos = positions[..., 1]
    first_traces = by_order(traces, order) * keep_mask[..., None]

    padded_movie = jnp.pad(movie, ((half_patch, half_patch), (half_patch, half_patch), (0, 0)))
    top_rows = (jnp.arange(tiles_down, dtype=jnp.int32) * tile_side)[:, None, None] + row_pos
    left_cols = (jnp.arange(tiles_across, dtype=jnp.int32) * tile_side)[None, :, None] + col_pos

    def window_drive(patch, top_row, left_col):
        window = lax.dynamic_slice(padded_movie, (top_row, left_col, jnp.int32(0)), (PATCH, PATCH, frame_count))
        return jnp.einsum('ij,ijf->f', patch.astype(jnp.float32), window.astype(jnp.float32), precision=precise)

    def tile_drive(items):
        return jax.vmap(window_drive)(items[0], items[1], items[2])

    drive_term = lax.map(tile_drive, (patches.reshape(-1, slot_count, PATCH, PATCH), top_rows.reshape(-1, slot_count), left_cols.reshape(-1, slot_count)))
    drive_term = drive_term.reshape(tiles_down, tiles_across, slot_count, frame_count)

    offsets = (jnp.arange(3, dtype=jnp.int32) - 1) * tile_side
    near_patch = neighbours(patches)
    near_rows = neighbours(row_pos) + jnp.repeat(offsets, 3)[None, None, :, None]
    near_cols = neighbours(col_pos) + jnp.tile(offsets, 3)[None, None, :, None]

    def tile_margins(items):
        own_patch, own_rows, own_cols, source_patch, source_rows, source_cols = items

        def per_source(source_items):
            return margin_rows(own_patch, own_rows, own_cols, source_items[0], source_items[1], source_items[2])

        return lax.map(per_source, (source_patch, source_rows, source_cols))

    margins = lax.map(tile_margins, (patches.reshape(-1, slot_count, PATCH, PATCH), row_pos.reshape(-1, slot_count), col_pos.reshape(-1, slot_count), near_patch.reshape(-1, 9, slot_count, PATCH, PATCH), near_rows.reshape(-1, 9, slot_count), near_cols.reshape(-1, 9, slot_count)))
    margins = margins.reshape(tiles_down, tiles_across, 9, slot_count, slot_count)

    current = first_traces.astype(jnp.float32)
    coupling = jnp.einsum('abnks,abnsf->abkf', margins, neighbours(current), precision=precise)
    diagonal = jnp.diagonal(margins[:, :, 4], axis1=2, axis2=3)
    denominator = jnp.where(alive_mask, diagonal, 1.0)
    for block_index in range(BLOCKS):
        lower = block_index * block_rows
        upper = lower + block_rows
        previous = current[:, :, lower:upper]
        renewed = jnp.maximum(previous + (drive_term[:, :, lower:upper] - coupling[:, :, lower:upper]) / denominator[:, :, lower:upper, None], 0.0)
        renewed = jnp.where(alive_mask[:, :, lower:upper, None], renewed, 0.0)
        current = current.at[:, :, lower:upper].set(renewed)
        if block_index + 1 < BLOCKS:
            change = neighbours(renewed - previous)
            coupling = coupling + jnp.einsum('abnks,abnsf->abkf', margins[..., lower:upper], change, precision=precise)
    inverse = jnp.argsort(order, axis=2).astype(jnp.int32)
    return jnp.take_along_axis(current, inverse[..., None], axis=2)
```

```python
import jax
import jax.numpy as jnp
from jax import lax
from jax.experimental import pallas as pl
from jax.experimental.pallas import tpu as pltpu
from jax.sharding import PartitionSpec as P

K = 32
F = 128
SIDE = 32
PIX = SIDE * SIDE
HALF = SIDE // 2
ROWS = 8
BLOCKS = 4
CHUNK = 16
MESH = pl.DeviceIdType.MESH
AROUND = [(u - 1, v - 1) for u in range(3) for v in range(3)]
f32, bf16, i32 = jnp.float32, jnp.bfloat16, jnp.int32
UP, DOWN, LEFT, RIGHT = (-1, 0), (1, 0), (0, -1), (0, 1)


def flip(o):
    return (-o[0], -o[1])


def slot_of(o):
    return (o[0] + 1) * 3 + o[1] + 1


def nt(x, y):
    return lax.dot_general(x, y, (((1,), (1,)), ((), ())), preferred_element_type=f32)


def nn(x, y):
    return jnp.dot(x, y, preferred_element_type=f32)


def exact(x, y):
    return jnp.dot(x, y, precision=lax.Precision.HIGHEST, preferred_element_type=f32)


def positive(x):
    return jnp.maximum(x, jnp.zeros_like(x))


def kernel(
    movie, foot_in, centres_in, traces_in, counts_in, order_in, out,
    foot, centres, traces, counts, order,
    top_movie, bottom_movie, to_left, to_right, to_up, to_down,
    from_right, from_left, from_down, from_up,
    start, start_up, start_down,
    sum_left, sum_right, sum_from_right, sum_from_left,
    cross_up, cross_down, cross_from_down, cross_from_up,
    change, changes,
    local_sem, send_sem, recv_sem,
):
    a, b = lax.axis_index("ty"), lax.axis_index("tx")
    n_ty, n_tx = lax.axis_size("ty"), lax.axis_size("tx")

    def there(o):
        row, col = a + o[0], b + o[1]
        return (row >= 0) & (row < n_ty) & (col >= 0) & (col < n_tx)

    barrier = pltpu.get_barrier_semaphore()
    expected = jnp.int32(0)
    for o in AROUND:
        if o == (0, 0):
            continue
        present = there(o)

        @pl.when(present)
        def _(o=o):
            pl.semaphore_signal(
                barrier, inc=1, device_id=(a + o[0], b + o[1]), device_id_type=MESH
            )

        expected = expected + present.astype(i32)

    local = []
    for source, target in (
        (order_in, order), (counts_in, counts), (centres_in, centres), (foot_in, foot),
        (traces_in, traces), (movie.at[pl.ds(0, HALF)], top_movie.at[pl.ds(0, HALF)]),
        (movie.at[pl.ds(HALF, HALF)], bottom_movie.at[pl.ds(HALF, HALF)]),
    ):
        copy = pltpu.make_async_copy(source, target, local_sem.at[len(local)])
        copy.start()
        local.append(copy)

    sent = []

    class Remote:
        def __init__(self, source, target, o):
            self.o = o
            index = len(sent)
            self.copy = pltpu.make_async_remote_copy(
                src_ref=source, dst_ref=target,
                send_sem=send_sem.at[index], recv_sem=recv_sem.at[index],
                device_id=(a + o[0], b + o[1]), device_id_type=MESH,
            )
            sent.append(self)

        def start(self):
            pl.when(there(self.o))(self.copy.start)
            return self

        def arrived(self):
            pl.when(there(flip(self.o)))(self.copy.wait_recv)

        def left(self):
            pl.when(there(self.o))(self.copy.wait_send)

    def clear(o, *refs):
        @pl.when(jnp.logical_not(there(o)))
        def _():
            for ref in refs:
                ref[...] = jnp.zeros_like(ref)

    clear(UP, from_up, start_up, cross_from_up, top_movie.at[pl.ds(HALF, HALF)])
    clear(DOWN, from_down, start_down, cross_from_down, bottom_movie.at[pl.ds(0, HALF)])
    clear(LEFT, from_left, sum_from_left)
    clear(RIGHT, from_right, sum_from_right)
    for o in AROUND:
        if o != (0, 0):
            clear(o, *[changes.at[q, slot_of(o)] for q in range(BLOCKS - 1)])

    for copy in local[:3]:
        copy.wait()
    sub = lax.broadcasted_iota(i32, (K, K), 0)
    lane = lax.broadcasted_iota(i32, (K, K), 1)
    order_row = order[0:1, :]
    alive_row = order_row < counts[0:1, 0:1]
    eye = sub == lane
    order_col = jnp.sum(
        jnp.where(eye, jnp.broadcast_to(order_row, (K, K)), 0).astype(f32), axis=1, keepdims=True
    ).astype(i32)
    alive_col = order_col < counts[0:1, 0:1]
    chooser = jnp.where((lane == order_col) & alive_col, 1.0, 0.0)
    back = jnp.where(sub == order_row, 1.0, 0.0)
    places = exact(chooser, centres[...].astype(f32)).astype(i32)
    row_at, col_at = places[:, 0:1], places[:, 1:2]
    for copy in local[3:5]:
        copy.wait()
    chooser16 = chooser.astype(bf16)
    ordered = nn(chooser16, foot[...])
    start_value = nn(chooser16, traces[...])
    start[...] = start_value.astype(bf16)

    lanes = lax.broadcasted_iota(i32, (K, F), 1)
    group, across = lanes >> 5, lanes & 31
    turn, shift = (row_at + HALF) & 31, (col_at + HALF) & 31
    fine, coarse = turn & 3, turn >> 2
    index = (((group - fine) & 3) << 5) + ((across - shift) & 31)
    slabs = [
        jnp.take_along_axis(ordered[:, v * F:(v + 1) * F], index, axis=1) for v in range(8)
    ]
    carry = group < fine
    slabs = [jnp.where(carry, slabs[(v - 1) % 8], slabs[v]) for v in range(8)]
    for bit in (1, 2, 4):
        taken = jnp.broadcast_to((coarse & bit) != 0, (K, F))
        slabs = [jnp.where(taken, slabs[(v - bit) % 8], slabs[v]) for v in range(8)]
    left_half = ((across + HALF) & 31) >= col_at
    for v in range(8):
        upper = ((4 * v + group + HALF) & 31) >= row_at
        x = slabs[v]
        by_row = jnp.where(upper, x, -x)
        by_col = jnp.where(left_half, x, -x)
        here = pl.ds(v * F, F)
        to_left[:, here] = jnp.where(left_half, by_row, 0.0).astype(bf16)
        to_right[:, here] = jnp.where(left_half, 0.0, by_row).astype(bf16)
        to_up[:, here] = jnp.where(upper, by_col, 0.0).astype(bf16)
        to_down[:, here] = jnp.where(upper, 0.0, by_col).astype(bf16)
    for copy in local[5:]:
        copy.wait()

    pl.semaphore_wait(barrier, expected)

    def part(ref, c):
        return ref.at[pl.ds(c * CHUNK, CHUNK)]

    side = [
        [Remote(part(to_left, c), part(from_right, c), LEFT),
         Remote(part(to_right, c), part(from_left, c), RIGHT)]
        for c in range(2)
    ]
    vertical = [
        Remote(to_up, from_down, UP), Remote(to_down, from_up, DOWN),
        Remote(start, start_down, UP), Remote(start, start_up, DOWN),
        Remote(top_movie.at[pl.ds(0, HALF)], bottom_movie.at[pl.ds(0, HALF)], UP),
        Remote(bottom_movie.at[pl.ds(HALF, HALF)], top_movie.at[pl.ds(HALF, HALF)], DOWN),
    ]
    for message in side[0] + vertical + side[1]:
        message.start()

    own_tl, own_bl = positive(to_left[...]), positive(-to_left[...])
    own_tr, own_br = positive(to_right[...]), positive(-to_right[...])
    pixel = lax.broadcasted_iota(i32, (K, PIX), 1) & 31
    near_side = jnp.where(pixel < HALF, 1.0, 0.0).astype(bf16)
    far_side = jnp.where(pixel < HALF, 0.0, 1.0).astype(bf16)
    for message in vertical:
        message.arrived()
    up_bl, up_br = positive(from_up[...]), positive(-from_up[...])
    down_tl, down_tr = positive(from_down[...]), positive(-from_down[...])
    above = top_movie[...].reshape(PIX, F)
    below = bottom_movie[...].reshape(PIX, F)
    s_own, s_up, s_down = (x[...].astype(f32) for x in (start, start_up, start_down))
    column_top = jnp.concatenate([s_own, s_up], axis=0)
    column_bottom = jnp.concatenate([s_own, s_down], axis=0)
    stack_tl = jnp.concatenate([own_tl, up_bl], axis=0)
    stack_tr = jnp.concatenate([own_tr, up_br], axis=0)
    stack_bl = jnp.concatenate([own_bl, down_tl], axis=0)
    stack_br = jnp.concatenate([own_br, down_tr], axis=0)

    own_top = nt(stack_tl, own_tl) + nt(stack_tr, own_tr)
    own_bottom = nt(stack_bl, own_bl) + nt(stack_br, own_br)
    own_own = own_top[:K] + own_bottom[:K]
    own_up, own_down = own_top[K:], own_bottom[K:]
    strip_top = own_tl * near_side + own_tr * far_side
    strip_bottom = own_bl * near_side + own_br * far_side
    total = nn(strip_top, above) + nn(strip_bottom, below)
    column = jnp.concatenate([own_own, own_up, own_down], axis=0)
    total = total - exact(column.T, jnp.concatenate([s_own, s_up, s_down], axis=0))
    diagonal = jnp.sum(jnp.where(eye, own_own, 0.0), axis=1, keepdims=True)
    divisor = jnp.where(alive_col, diagonal, 1.0)

    returns, grams = [], []
    for c in range(2):
        for message in side[c]:
            message.arrived()
        from_l, from_r = part(from_left, c)[...], part(from_right, c)[...]
        l_tr, l_br = positive(from_l), positive(-from_l)
        r_tl, r_bl = positive(from_r), positive(-from_r)
        gram_tl, gram_bl = nt(l_tr, stack_tl), nt(l_br, stack_bl)
        gram_tr, gram_br = nt(r_tl, stack_tr), nt(r_bl, stack_br)
        grams.append((gram_tl, gram_bl, gram_tr, gram_br))
        near, far = near_side[:CHUNK], far_side[:CHUNK]
        upper = jnp.concatenate([l_tr * near, r_tl * far], axis=0)
        lower = jnp.concatenate([l_br * near, r_bl * far], axis=0)
        both = nn(upper, above) + nn(lower, below)
        both = both - exact(jnp.concatenate([gram_tl, gram_tr], axis=0), column_top)
        both = both - exact(jnp.concatenate([gram_bl, gram_br], axis=0), column_bottom)
        part(sum_left, c)[...] = both[:CHUNK]
        part(sum_right, c)[...] = both[CHUNK:]
        pair = [
            Remote(part(sum_left, c), part(sum_from_right, c), LEFT).start(),
            Remote(part(sum_right, c), part(sum_from_left, c), RIGHT).start(),
        ]
        returns.append(pair)
    gram_tl, gram_bl, gram_tr, gram_br = (jnp.concatenate(g, axis=0) for g in zip(*grams))
    cross_up[...] = jnp.concatenate([gram_tl[:, K:], gram_tr[:, K:]], axis=0)
    cross_down[...] = jnp.concatenate([gram_bl[:, K:], gram_br[:, K:]], axis=0)
    crossing = [
        Remote(cross_up, cross_from_down, UP).start(),
        Remote(cross_down, cross_from_up, DOWN).start(),
    ]
    own_left = gram_tl[:, :K] + gram_bl[:, :K]
    own_right = gram_tr[:, :K] + gram_br[:, :K]
    for message in crossing:
        message.arrived()
    around = [
        cross_from_up[:K, :], own_up, cross_from_up[K:, :],
        own_left, own_own, own_right,
        cross_from_down[:K, :], own_down, cross_from_down[K:, :],
    ]
    columns = [
        jnp.concatenate([m[q * ROWS:(q + 1) * ROWS] for m in around], axis=0).T
        for q in range(BLOCKS - 1)
    ]

    current = []
    for q in range(BLOCKS):
        if q % 2 == 0:
            for message in returns[q // 2]:
                message.arrived()
        rows = slice(q * ROWS, (q + 1) * ROWS)
        if q % 2 == 0:
            pair_rows = slice(q * ROWS, (q + 2) * ROWS)
            gathered = sum_from_left[pair_rows, :] + sum_from_right[pair_rows, :]
            total = jnp.concatenate(
                [total[:q * ROWS]] * (q > 0)
                + [total[pair_rows] + gathered]
                + [total[(q + 2) * ROWS:]] * (q + 2 < BLOCKS),
                axis=0,
            )
        previous = start_value[rows]
        renewed = jnp.maximum(previous + total[rows] / divisor[rows], 0.0)
        renewed = jnp.where(alive_col[rows], renewed, 0.0)
        current.append(renewed)
        if q + 1 == BLOCKS:
            break
        mine = renewed - previous
        change[q] = mine
        messages = [
            Remote(change.at[q], changes.at[q, slot_of(flip(o))], o).start()
            for o in AROUND if o != (0, 0)
        ]
        for message in messages:
            message.arrived()
        moved = jnp.concatenate(
            [mine if n == 4 else changes[q, n] for n in range(9)], axis=0
        )
        total = total - exact(columns[q], moved)
    out[...] = exact(back, jnp.concatenate(current, axis=0))
    for message in sent:
        message.left()


def body(movie, footprints, centres, traces, counts, order):
    messages = 4 + 6 + 4 + 2 + 8 * (BLOCKS - 1)
    any_space = pl.BlockSpec(memory_space=pl.ANY)
    result = pl.pallas_call(
        kernel,
        name="hals",
        out_shape=jax.ShapeDtypeStruct((K, F), f32),
        in_specs=[any_space] * 6,
        out_specs=pl.BlockSpec(memory_space=pltpu.VMEM),
        scratch_shapes=[
            pltpu.VMEM((K, PIX), bf16), pltpu.VMEM((K, 2), i32), pltpu.VMEM((K, F), bf16),
            pltpu.VMEM((1, 1), i32), pltpu.VMEM((1, K), i32),
            pltpu.VMEM((SIDE, SIDE, F), bf16), pltpu.VMEM((SIDE, SIDE, F), bf16),
            *[pltpu.VMEM((K, PIX), bf16) for _ in range(8)],
            *[pltpu.VMEM((K, F), bf16) for _ in range(3)],
            *[pltpu.VMEM((K, F), f32) for _ in range(4)],
            *[pltpu.VMEM((2 * K, K), f32) for _ in range(4)],
            pltpu.VMEM((BLOCKS - 1, ROWS, F), f32), pltpu.VMEM((BLOCKS - 1, 9, ROWS, F), f32),
            pltpu.SemaphoreType.DMA((7,)),
            pltpu.SemaphoreType.DMA((messages,)), pltpu.SemaphoreType.DMA((messages,)),
        ],
        compiler_params=pltpu.CompilerParams(collective_id=0, has_side_effects=True),
    )(movie, footprints[0, 0], centres[0, 0], traces[0, 0], counts, order[0])
    return result[None, None]


def solution(mesh):
    in_specs = (
        P("ty", "tx", None),
        P("ty", "tx", None, None),
        P("ty", "tx", None, None),
        P("ty", "tx", None, None),
        P("ty", "tx"),
        P("ty", "tx", None),
    )
    out_specs = P("ty", "tx", None, None)
    return jax.shard_map(body, mesh=mesh, in_specs=in_specs, out_specs=out_specs, check_vma=False)
```

```python
import jax
import jax.numpy as jnp
from jax import lax
from jax.experimental import pallas as pl
from jax.experimental.pallas import tpu as pltpu
from jax.sharding import PartitionSpec as P

K = 32
F = 128
SIDE = 32
PIX = SIDE * SIDE
HALF = SIDE // 2
ROWS = 8
BLOCKS = 4
FIRST = 24
MESH = pl.DeviceIdType.MESH
NEAR = [(u, v) for u in (-1, 0, 1) for v in (-1, 0, 1)]
WIDE = [(u, v) for u in range(-2, 3) for v in range(-2, 3)]
RING = [o for o in WIDE if o not in NEAR]
BAND = [(u, v) for u in (-1, 0, 1) for v in range(-2, 3) if (u, v) != (0, 0)]
HERE = (0, 0)
f32, bf16, i32 = jnp.float32, jnp.bfloat16, jnp.int32
UP, DOWN, LEFT, RIGHT = (-1, 0), (1, 0), (0, -1), (0, 1)


def flip(o):
    return (-o[0], -o[1])


def plus(o, p):
    return (o[0] + p[0], o[1] + p[1])


def nt(x, y):
    return lax.dot_general(x, y, (((1,), (1,)), ((), ())), preferred_element_type=f32)


def tn(x, y):
    return lax.dot_general(x, y, (((0,), (0,)), ((), ())), preferred_element_type=f32)


def nn(x, y):
    return jnp.dot(x, y, preferred_element_type=f32)


def rounded(x):
    return x.astype(bf16).astype(f32)


def lanes_of(x):
    high = rounded(x)
    return jnp.concatenate([high, high, x - high], axis=1).astype(bf16)


def rows_of(x):
    high = rounded(x)
    return jnp.concatenate([high, x - high, high], axis=0).astype(bf16)


def positive(x):
    return jnp.maximum(x, jnp.zeros_like(x))


def kernel(
    movie, foot_in, centres_in, traces_in, counts_in, order_in, out,
    foot, centres, traces, counts, order,
    top_movie, bottom_movie, to_left, to_right, to_up, to_down,
    from_right, from_left, from_down, from_up,
    start, start_up, start_down, info, infos,
    about, abouts, sum_left, sum_right, sum_from_right, sum_from_left,
    cross_up, cross_down, cross_from_down, cross_from_up,
    margin, margins, step, steps, far_steps,
    local_sem, send_sem, recv_sem,
):
    a, b = lax.axis_index("ty"), lax.axis_index("tx")
    n_ty, n_tx = lax.axis_size("ty"), lax.axis_size("tx")

    def there(o):
        row, col = a + o[0], b + o[1]
        return (row >= 0) & (row < n_ty) & (col >= 0) & (col < n_tx)

    barrier = pltpu.get_barrier_semaphore()
    expected = jnp.int32(0)
    for o in WIDE:
        if o == HERE:
            continue
        present = there(o)

        @pl.when(present)
        def _(o=o):
            pl.semaphore_signal(
                barrier, inc=1, device_id=(a + o[0], b + o[1]), device_id_type=MESH
            )

        expected = expected + present.astype(i32)

    local = []
    for source, target in (
        (order_in, order), (counts_in, counts), (centres_in, centres), (foot_in, foot),
        (traces_in, traces), (movie.at[pl.ds(0, HALF)], top_movie.at[pl.ds(0, HALF)]),
        (movie.at[pl.ds(HALF, HALF)], bottom_movie.at[pl.ds(HALF, HALF)]),
    ):
        copy = pltpu.make_async_copy(source, target, local_sem.at[len(local)])
        copy.start()
        local.append(copy)

    sent = []

    class Remote:
        def __init__(self, source, target, o):
            self.o = o
            index = len(sent)
            self.copy = pltpu.make_async_remote_copy(
                src_ref=source, dst_ref=target,
                send_sem=send_sem.at[index], recv_sem=recv_sem.at[index],
                device_id=(a + o[0], b + o[1]), device_id_type=MESH,
            )
            sent.append(self)

        def start(self):
            pl.when(there(self.o))(self.copy.start)
            return self

        def arrived(self):
            pl.when(there(flip(self.o)))(self.copy.wait_recv)

        def left(self):
            pl.when(there(self.o))(self.copy.wait_send)

    def clear(o, *refs):
        @pl.when(jnp.logical_not(there(o)))
        def _():
            for ref in refs:
                ref[...] = jnp.zeros_like(ref)

    def slot(o):
        return (o[0] + 1) * 3 + o[1] + 1

    clear(UP, from_up, start_up, cross_from_up, top_movie.at[pl.ds(HALF, HALF)])
    clear(DOWN, from_down, start_down, cross_from_down, bottom_movie.at[pl.ds(0, HALF)])
    clear(LEFT, from_left, sum_from_left)
    clear(RIGHT, from_right, sum_from_right)
    for o in NEAR:
        if o != HERE:
            clear(o, infos.at[slot(o)], margins.at[slot(o)], steps.at[slot(o)])
    for o in BAND:
        clear(o, abouts.at[o[0] + 1, o[1] + 2])
    for o in RING:
        clear(o, far_steps.at[RING.index(o)])

    for copy in local[:3]:
        copy.wait()
    sub = lax.broadcasted_iota(i32, (K, K), 0)
    lane = lax.broadcasted_iota(i32, (K, K), 1)

    def to_column(row, pick):
        spread = jnp.where(pick, jnp.broadcast_to(row, (K, K)), 0)
        return jnp.sum(spread.astype(f32), axis=1, keepdims=True)

    order_row = order[0:1, :]
    order_col = to_column(order_row, sub == lane).astype(i32)
    alive_col = order_col < counts[0:1, 0:1]
    picked = (lane == order_col) & alive_col
    row_at = to_column(centres[0:1, :], picked).astype(i32)
    col_at = to_column(centres[1:2, :], picked).astype(i32)
    for copy in local[3:5]:
        copy.wait()
    chooser = jnp.where(picked, 1.0, 0.0).astype(bf16)
    ordered = nn(chooser, foot[...])
    start_value = nn(chooser, traces[...])
    start[...] = start_value.astype(bf16)
    diagonal = jnp.sum(ordered * ordered, axis=1, keepdims=True)
    divisor = jnp.where(alive_col, diagonal, 1.0)
    level = jnp.broadcast_to(divisor, (K, F))
    level_high = rounded(level)
    level_mid = rounded(level - level_high)
    level_low = level - level_high - level_mid
    wide_lane = lax.broadcasted_iota(i32, (K, F), 1)
    level_parts = jnp.where(
        wide_lane == 0, level_high, jnp.where(wide_lane == 1, level_mid, level_low)
    )
    info[...] = jnp.concatenate(
        [start_value[:ROWS], start_value[2 * ROWS:3 * ROWS],
         level_parts[:ROWS], level_parts[2 * ROWS:3 * ROWS]], axis=0
    ).astype(bf16)

    group, across = wide_lane >> 5, wide_lane & 31
    turn, shift = (row_at + HALF) & 31, (col_at + HALF) & 31
    fine, coarse = turn & 3, turn >> 2
    index = (((group - fine) & 3) << 5) + ((across - shift) & 31)
    slabs = [
        jnp.take_along_axis(ordered[:, v * F:(v + 1) * F], index, axis=1) for v in range(8)
    ]
    carry = group < fine
    slabs = [jnp.where(carry, slabs[(v - 1) % 8], slabs[v]) for v in range(8)]
    for bit in (1, 2, 4):
        taken = jnp.broadcast_to((coarse & bit) != 0, (K, F))
        slabs = [jnp.where(taken, slabs[(v - bit) % 8], slabs[v]) for v in range(8)]
    left_half = ((across + HALF) & 31) >= col_at
    for v in range(8):
        upper = ((4 * v + group + HALF) & 31) >= row_at
        x = slabs[v]
        by_row = jnp.where(upper, x, -x)
        by_col = jnp.where(left_half, x, -x)
        here = pl.ds(v * F, F)
        to_left[:, here] = jnp.where(left_half, by_row, 0.0).astype(bf16)
        to_right[:, here] = jnp.where(left_half, 0.0, by_row).astype(bf16)
        to_up[:, here] = jnp.where(upper, by_col, 0.0).astype(bf16)
        to_down[:, here] = jnp.where(upper, 0.0, by_col).astype(bf16)
    for copy in local[5:]:
        copy.wait()

    pl.semaphore_wait(barrier, expected)

    early, late = pl.ds(0, FIRST), pl.ds(FIRST, K - FIRST)
    side, side_late = [
        [Remote(to_left.at[rows], from_right.at[rows], LEFT),
         Remote(to_right.at[rows], from_left.at[rows], RIGHT)]
        for rows in (early, late)
    ]
    vertical = [
        Remote(to_up, from_down, UP), Remote(to_down, from_up, DOWN),
        Remote(start, start_down, UP), Remote(start, start_up, DOWN),
        Remote(top_movie.at[pl.ds(0, HALF)], bottom_movie.at[pl.ds(0, HALF)], UP),
        Remote(bottom_movie.at[pl.ds(HALF, HALF)], top_movie.at[pl.ds(HALF, HALF)], DOWN),
    ]
    known = [Remote(info, infos.at[slot(flip(o))], o) for o in NEAR if o != HERE]
    for message in side + vertical + side_late + known:
        message.start()

    own_tl, own_bl = positive(to_left[...]), positive(-to_left[...])
    own_tr, own_br = positive(to_right[...]), positive(-to_right[...])
    for message in vertical:
        message.arrived()
    up_bl, up_br = positive(from_up[...]), positive(-from_up[...])
    down_tl, down_tr = positive(from_down[...]), positive(-from_down[...])
    column_top = jnp.concatenate([start[...], start_up[...]], axis=0)
    column_bottom = jnp.concatenate([start[...], start_down[...]], axis=0)
    stack_tl = jnp.concatenate([own_tl, up_bl], axis=0)
    stack_tr = jnp.concatenate([own_tr, up_br], axis=0)
    stack_bl = jnp.concatenate([own_bl, down_tl], axis=0)
    stack_br = jnp.concatenate([own_br, down_tr], axis=0)

    near_rows = (lax.broadcasted_iota(i32, (PIX, F), 0) & 31) < HALF

    def residual(pixels, near, stack, column):
        seen = pixels[...].reshape(PIX, F).astype(f32)
        seen = jnp.where(near_rows, seen, 0.0) if near else jnp.where(near_rows, 0.0, seen)
        rest = seen - tn(stack, column)
        high = rounded(rest)
        return jnp.concatenate([high, rest - high], axis=1).astype(bf16)

    rest_tl = residual(top_movie, True, stack_tl, column_top)
    rest_tr = residual(top_movie, False, stack_tr, column_top)
    rest_bl = residual(bottom_movie, True, stack_bl, column_bottom)
    rest_br = residual(bottom_movie, False, stack_br, column_bottom)
    both = nn(own_tl, rest_tl) + nn(own_tr, rest_tr) + nn(own_bl, rest_bl) + nn(own_br, rest_br)
    total = both[:, :F] + both[:, F:]

    def halves(rows):
        l, r = from_left[rows, :], from_right[rows, :]
        return positive(l), positive(-l), positive(r), positive(-r)

    def side_sums(l_tr, l_br, r_tl, r_bl):
        l = nn(l_tr, rest_tl) + nn(l_br, rest_bl)
        r = nn(r_tl, rest_tr) + nn(r_bl, rest_br)
        return l[:, :F] + l[:, F:], r[:, :F] + r[:, F:]

    for message in side:
        message.arrived()
    parts = halves(early)
    l_sum, r_sum = side_sums(*parts)
    about[0], about[1], about[2] = l_sum[:ROWS], total[:ROWS], r_sum[:ROWS]
    sum_left[:FIRST, :], sum_right[:FIRST, :] = l_sum, r_sum
    first_sums = []
    for o in BAND:
        low, high = max(0, o[1]), min(3, 3 + o[1])
        first_sums.append(
            Remote(
                about.at[pl.ds(low, high - low)],
                abouts.at[1 - o[0], 2 - o[1], pl.ds(low - o[1], high - low)], o,
            ).start()
        )
    middle = pl.ds(ROWS, FIRST - ROWS)
    returned = [
        Remote(sum_left.at[middle], sum_from_right.at[middle], LEFT).start(),
        Remote(sum_right.at[middle], sum_from_left.at[middle], RIGHT).start(),
    ]

    l_tr, l_br, r_tl, r_bl = parts
    gram_tl, gram_bl = nt(l_tr, stack_tl), nt(l_br, stack_bl)
    gram_tr, gram_br = nt(r_tl, stack_tr), nt(r_bl, stack_br)
    cross_up[...] = jnp.concatenate([gram_tl[:, K:], gram_tr[:, K:]], axis=0)
    cross_down[...] = jnp.concatenate([gram_bl[:, K:], gram_br[:, K:]], axis=0)
    crossing = [
        Remote(cross_up, cross_from_down, UP).start(),
        Remote(cross_down, cross_from_up, DOWN).start(),
    ]
    own_left = gram_tl[:, :K] + gram_bl[:, :K]
    own_right = gram_tr[:, :K] + gram_br[:, :K]
    own_top = nt(stack_tl, own_tl) + nt(stack_tr, own_tr)
    own_bottom = nt(stack_bl, own_bl) + nt(stack_br, own_br)
    own_own = own_top[:K] + own_bottom[:K]
    own_up, own_down = own_top[K:], own_bottom[K:]

    for message in side_late:
        message.arrived()
    l_sum, r_sum = side_sums(*halves(late))
    sum_left[FIRST:, :], sum_right[FIRST:, :] = l_sum, r_sum
    returned_late = [
        Remote(sum_left.at[late], sum_from_right.at[late], LEFT).start(),
        Remote(sum_right.at[late], sum_from_left.at[late], RIGHT).start(),
    ]

    for message in crossing:
        message.arrived()
    around = [
        cross_from_up[:FIRST, :], own_up, cross_from_up[FIRST:, :],
        own_left, own_own, own_right,
        cross_from_down[:FIRST, :], own_down, cross_from_down[FIRST:, :],
    ]
    columns = [
        jnp.concatenate([m[q * ROWS:(q + 1) * ROWS] for m in around], axis=0).T
        for q in range(BLOCKS - 1)
    ]
    margin[...] = columns[1][2 * ROWS:3 * ROWS]
    lent = [Remote(margin, margins.at[slot(flip(o))], o).start() for o in NEAR if o != HERE]
    columns = [lanes_of(x) for x in columns]

    def stepped(previous, left_over, level):
        return jnp.maximum(previous + left_over / level, 0.0)

    def rows(q):
        return slice(q * ROWS, (q + 1) * ROWS)

    for message in known:
        message.arrived()
    facts = {}
    for o in NEAR:
        if o == HERE:
            facts[o] = [start_value[rows(0)], start_value[rows(2)], divisor[rows(0)], divisor[rows(2)]]
            continue
        x = infos[slot(o)].astype(f32)
        level = x[:, 0:1] + x[:, 1:2] + x[:, 2:3]
        levels = (jnp.where(y == 0.0, 1.0, y) for y in (level[rows(2)], level[rows(3)]))
        facts[o] = [x[rows(0)], x[rows(1)], *levels]

    for message in first_sums:
        message.arrived()
    moved = []
    for o in NEAR:
        left_over = None
        for v in range(-2, 3):
            if abs(v - o[1]) > 1:
                continue
            piece = (
                about[o[1] + 1] if (o[0], v) == HERE
                else abouts[o[0] + 1, v + 2, o[1] + 1]
            )
            left_over = piece if left_over is None else left_over + piece
        previous = facts[o][0]
        renewed = stepped(previous, left_over, facts[o][2])
        if o == HERE:
            renewed = jnp.where(alive_col[rows(0)], renewed, 0.0)
            current = [renewed]
        moved.append(renewed - previous)
    for message in returned:
        message.arrived()
    total = total[ROWS:FIRST] + sum_from_left[ROWS:FIRST, :] + sum_from_right[ROWS:FIRST, :]
    change = nn(columns[0][ROWS:], rows_of(jnp.concatenate(moved, axis=0)))
    total = total - change[:FIRST - ROWS]

    previous = start_value[rows(1)]
    renewed = stepped(previous, total[:ROWS], divisor[rows(1)])
    renewed = jnp.where(alive_col[rows(1)], renewed, 0.0)
    current.append(renewed)
    own_step = renewed - previous
    step[:ROWS, :] = own_step
    step[ROWS:, :] = total[ROWS:]
    moves = [
        Remote(step, steps.at[slot(flip(o))], o).start() if o in NEAR
        else Remote(
            step.at[pl.ds(0, ROWS)], far_steps.at[RING.index(flip(o))], o
        ).start()
        for o in WIDE if o != HERE
    ]
    for message in returned_late:
        message.arrived()
    last = both[FIRST:, :F] + both[FIRST:, F:] + sum_from_left[FIRST:, :]
    last = last + sum_from_right[FIRST:, :] - change[FIRST - ROWS:]
    for message in lent:
        message.arrived()
    weights = {
        o: lanes_of(margin[...] if o == HERE else margins[slot(o)]) for o in NEAR
    }

    for message in moves:
        message.arrived()
    taken = {
        o: own_step if o == HERE
        else steps[slot(o), :ROWS, :] if o in NEAR
        else far_steps[RING.index(o)]
        for o in WIDE
    }
    moved = []
    for o in NEAR:
        nearby = rows_of(jnp.concatenate([taken[plus(o, p)] for p in NEAR], axis=0))
        if o == HERE:
            left_over = total[ROWS:]
            last = last - nn(columns[1][FIRST:], nearby)
        else:
            left_over = steps[slot(o), ROWS:, :]
        left_over = left_over - nn(weights[o], nearby)
        previous = facts[o][1]
        renewed = stepped(previous, left_over, facts[o][3])
        if o == HERE:
            renewed = jnp.where(alive_col[rows(2)], renewed, 0.0)
            current.append(renewed)
        moved.append(renewed - previous)

    last = last - nn(columns[2][FIRST:], rows_of(jnp.concatenate(moved, axis=0)))
    renewed = stepped(start_value[rows(3)], last, divisor[rows(3)])
    current.append(jnp.where(alive_col[rows(3)], renewed, 0.0))
    result = jnp.concatenate(current, axis=0)
    high = rounded(result)
    mid = rounded(result - high)
    back = jnp.where(sub == order_row, 1.0, 0.0)
    out[...] = nn(
        jnp.concatenate([back, back, back], axis=1).astype(bf16),
        jnp.concatenate([high, mid, result - high - mid], axis=0).astype(bf16),
    )
    for message in sent:
        message.left()


def body(movie, footprints, centres, traces, counts, order):
    messages = 4 + 6 + 8 + len(BAND) + 4 + 2 + 8 + 24
    any_space = pl.BlockSpec(memory_space=pl.ANY)
    result = pl.pallas_call(
        kernel,
        name="hals",
        out_shape=pltpu.VMEM((K, F), f32),
        in_specs=[any_space] * 6,
        out_specs=pl.BlockSpec(memory_space=pltpu.VMEM),
        scratch_shapes=[
            pltpu.VMEM((K, PIX), bf16), pltpu.VMEM((2, K), i32), pltpu.VMEM((K, F), bf16),
            pltpu.VMEM((1, 1), i32), pltpu.VMEM((1, K), i32),
            pltpu.VMEM((SIDE, SIDE, F), bf16), pltpu.VMEM((SIDE, SIDE, F), bf16),
            *[pltpu.VMEM((K, PIX), bf16) for _ in range(8)],
            *[pltpu.VMEM((K, F), bf16) for _ in range(4)], pltpu.VMEM((9, K, F), bf16),
            pltpu.VMEM((3, ROWS, F), f32), pltpu.VMEM((3, 5, 3, ROWS, F), f32),
            *[pltpu.VMEM((K, F), f32) for _ in range(4)],
            *[pltpu.VMEM((2 * FIRST, K), f32) for _ in range(4)],
            pltpu.VMEM((ROWS, 9 * ROWS), f32), pltpu.VMEM((9, ROWS, 9 * ROWS), f32),
            pltpu.VMEM((2 * ROWS, F), f32), pltpu.VMEM((9, 2 * ROWS, F), f32),
            pltpu.VMEM((len(RING), ROWS, F), f32),
            pltpu.SemaphoreType.DMA((7,)),
            pltpu.SemaphoreType.DMA((messages,)), pltpu.SemaphoreType.DMA((messages,)),
        ],
        compiler_params=pltpu.CompilerParams(collective_id=0, has_side_effects=True),
    )(movie, footprints[0, 0], centres[0, 0].T, traces[0, 0], counts, order[0])
    return result[None, None]


def solution(mesh):
    in_specs = (
        P("ty", "tx", None),
        P("ty", "tx", None, None),
        P("ty", "tx", None, None),
        P("ty", "tx", None, None),
        P("ty", "tx"),
        P("ty", "tx", None),
    )
    out_specs = P("ty", "tx", None, None)
    return jax.shard_map(body, mesh=mesh, in_specs=in_specs, out_specs=out_specs, check_vma=False)
```

```python
import jax
import jax.numpy as jnp
from jax import lax
from jax.experimental import pallas as pl
from jax.experimental.pallas import tpu as pltpu
from jax.sharding import PartitionSpec as P

K = 32
F = 128
SIDE = 32
PIX = SIDE * SIDE
HALF = SIDE // 2
ROWS = 8
BLOCKS = 4
MESH = pl.DeviceIdType.MESH
NEAR = [(u, v) for u in (-1, 0, 1) for v in (-1, 0, 1)]
WIDE = [(u, v) for u in range(-2, 3) for v in range(-2, 3)]
RING = [o for o in WIDE if o not in NEAR]
BAND = [(u, v) for v in (-1, 1, -2, 2, 0) for u in (0, -1, 1) if (u, v) != (0, 0)]
OUTWARD = [(u, v) for v in (-1, 1, -2, 2, 0) for u in (0, -1, 1, -2, 2) if (u, v) != (0, 0)]
HERE = (0, 0)
f32, bf16, i32 = jnp.float32, jnp.bfloat16, jnp.int32
UP, DOWN, LEFT, RIGHT = (-1, 0), (1, 0), (0, -1), (0, 1)


def flip(o):
    return (-o[0], -o[1])


def plus(o, p):
    return (o[0] + p[0], o[1] + p[1])


def nt(x, y):
    return lax.dot_general(x, y, (((1,), (1,)), ((), ())), preferred_element_type=f32)


def tn(x, y):
    return lax.dot_general(x, y, (((0,), (0,)), ((), ())), preferred_element_type=f32)


def nn(x, y):
    return jnp.dot(x, y, preferred_element_type=f32)


def rounded(x):
    return x.astype(bf16).astype(f32)


def lanes_of(x):
    high = rounded(x)
    return jnp.concatenate([high, high, x - high], axis=1).astype(bf16)


def rows_of(x):
    high = rounded(x)
    return jnp.concatenate([high, x - high, high], axis=0).astype(bf16)


def positive(x):
    return jnp.maximum(x, jnp.zeros_like(x))


def kernel(
    movie, foot_in, centres_in, traces_in, counts_in, order_in, out,
    foot, centres, traces, counts, order,
    top_movie, bottom_movie, to_left, to_right, to_up, to_down,
    from_right, from_left, from_down, from_up,
    start, start_up, start_down, info, infos,
    about, abouts, sum_left, sum_right, sum_from_right, sum_from_left,
    cross_up, cross_down, cross_from_down, cross_from_up,
    margin, margins, step, steps, far_steps,
    local_sem, send_sem, recv_sem,
):
    a, b = lax.axis_index("ty"), lax.axis_index("tx")
    n_ty, n_tx = lax.axis_size("ty"), lax.axis_size("tx")

    def there(o):
        row, col = a + o[0], b + o[1]
        return (row >= 0) & (row < n_ty) & (col >= 0) & (col < n_tx)

    barrier = pltpu.get_barrier_semaphore()
    expected = jnp.int32(0)
    for o in NEAR:
        if o == HERE:
            continue
        present = there(o)

        @pl.when(present)
        def _(o=o):
            pl.semaphore_signal(
                barrier, inc=1, device_id=(a + o[0], b + o[1]), device_id_type=MESH
            )

        expected = expected + present.astype(i32)

    local = []
    for source, target in (
        (order_in, order), (counts_in, counts), (centres_in, centres), (foot_in, foot),
        (traces_in, traces), (movie.at[pl.ds(0, HALF)], top_movie.at[pl.ds(0, HALF)]),
        (movie.at[pl.ds(HALF, HALF)], bottom_movie.at[pl.ds(HALF, HALF)]),
    ):
        copy = pltpu.make_async_copy(source, target, local_sem.at[len(local)])
        copy.start()
        local.append(copy)

    sent = []

    class Remote:
        def __init__(self, source, target, o):
            self.o = o
            index = len(sent)
            self.copy = pltpu.make_async_remote_copy(
                src_ref=source, dst_ref=target,
                send_sem=send_sem.at[index], recv_sem=recv_sem.at[index],
                device_id=(a + o[0], b + o[1]), device_id_type=MESH,
            )
            sent.append(self)

        def start(self):
            pl.when(there(self.o))(self.copy.start)
            return self

        def arrived(self):
            pl.when(there(flip(self.o)))(self.copy.wait_recv)

        def left(self):
            pl.when(there(self.o))(self.copy.wait_send)

    def clear(o, *refs):
        @pl.when(jnp.logical_not(there(o)))
        def _():
            for ref in refs:
                ref[...] = jnp.zeros_like(ref)

    def slot(o):
        return (o[0] + 1) * 3 + o[1] + 1

    clear(UP, from_up, start_up, cross_from_up, top_movie.at[pl.ds(HALF, HALF)])
    clear(DOWN, from_down, start_down, cross_from_down, bottom_movie.at[pl.ds(0, HALF)])
    clear(LEFT, from_left, sum_from_left)
    clear(RIGHT, from_right, sum_from_right)
    for o in NEAR:
        if o != HERE:
            clear(o, infos.at[0, slot(o)], infos.at[1, slot(o)], margins.at[slot(o)])
            clear(o, steps.at[slot(o)])
    for o in BAND:
        clear(o, *[abouts.at[i, o[0] + 1, o[1] + 2] for i in range(2)])
    for o in RING:
        clear(o, far_steps.at[RING.index(o)])

    for copy in local[:3]:
        copy.wait()
    sub = lax.broadcasted_iota(i32, (K, K), 0)
    lane = lax.broadcasted_iota(i32, (K, K), 1)

    def to_column(row, pick):
        spread = jnp.where(pick, jnp.broadcast_to(row, (K, K)), 0)
        return jnp.sum(spread.astype(f32), axis=1, keepdims=True)

    order_row = order[0:1, :]
    order_col = to_column(order_row, sub == lane).astype(i32)
    alive_col = order_col < counts[0:1, 0:1]
    picked = (lane == order_col) & alive_col
    row_at = to_column(centres[0:1, :], picked).astype(i32)
    col_at = to_column(centres[1:2, :], picked).astype(i32)
    for copy in local[3:5]:
        copy.wait()
    chooser = jnp.where(picked, 1.0, 0.0).astype(bf16)
    ordered = nn(chooser, foot[...])
    start_value = nn(chooser, traces[...])
    start[...] = start_value.astype(bf16)
    diagonal = jnp.sum(ordered * ordered, axis=1, keepdims=True)
    divisor = jnp.where(alive_col, diagonal, 1.0)
    level = jnp.broadcast_to(divisor, (K, F))
    level_high = rounded(level)
    level_mid = rounded(level - level_high)
    level_low = level - level_high - level_mid
    wide_lane = lax.broadcasted_iota(i32, (K, F), 1)
    level_parts = jnp.where(
        wide_lane == 0, level_high, jnp.where(wide_lane == 1, level_mid, level_low)
    )
    for i, q in enumerate((0, 2)):
        info[i] = jnp.concatenate(
            [x[q * ROWS:(q + 1) * ROWS] for x in (start_value, level_parts)], axis=0
        ).astype(bf16)

    group, across = wide_lane >> 5, wide_lane & 31
    turn, shift = (row_at + HALF) & 31, (col_at + HALF) & 31
    fine, coarse = turn & 3, turn >> 2
    index = (((group - fine) & 3) << 5) + ((across - shift) & 31)
    slabs = [
        jnp.take_along_axis(ordered[:, v * F:(v + 1) * F], index, axis=1) for v in range(8)
    ]
    carry = group < fine
    slabs = [jnp.where(carry, slabs[(v - 1) % 8], slabs[v]) for v in range(8)]
    for bit in (1, 2, 4):
        taken = jnp.broadcast_to((coarse & bit) != 0, (K, F))
        slabs = [jnp.where(taken, slabs[(v - bit) % 8], slabs[v]) for v in range(8)]
    left_half = ((across + HALF) & 31) >= col_at
    for v in range(8):
        upper = ((4 * v + group + HALF) & 31) >= row_at
        x = slabs[v]
        by_row = jnp.where(upper, x, -x)
        by_col = jnp.where(left_half, x, -x)
        here = pl.ds(v * F, F)
        to_left[:, here] = jnp.where(left_half, by_row, 0.0).astype(bf16)
        to_right[:, here] = jnp.where(left_half, 0.0, by_row).astype(bf16)
        to_up[:, here] = jnp.where(upper, by_col, 0.0).astype(bf16)
        to_down[:, here] = jnp.where(upper, 0.0, by_col).astype(bf16)
    for copy in local[5:]:
        copy.wait()

    pl.semaphore_wait(barrier, expected)

    def chunk(q):
        return pl.ds(q * ROWS, ROWS)

    side = [
        [Remote(to_left.at[chunk(q)], from_right.at[chunk(q)], LEFT),
         Remote(to_right.at[chunk(q)], from_left.at[chunk(q)], RIGHT)]
        for q in range(BLOCKS)
    ]
    vertical = [
        Remote(to_up, from_down, UP), Remote(to_down, from_up, DOWN),
        Remote(start, start_down, UP), Remote(start, start_up, DOWN),
        Remote(top_movie.at[pl.ds(0, HALF)], bottom_movie.at[pl.ds(0, HALF)], UP),
        Remote(bottom_movie.at[pl.ds(HALF, HALF)], top_movie.at[pl.ds(HALF, HALF)], DOWN),
    ]
    known = [
        [Remote(info.at[i], infos.at[i, slot(flip(o))], o) for o in NEAR if o != HERE]
        for i in range(2)
    ]
    for message in side[0] + side[1] + vertical + side[2] + known[0]:
        message.start()

    own_tl, own_bl = positive(to_left[...]), positive(-to_left[...])
    own_tr, own_br = positive(to_right[...]), positive(-to_right[...])
    for message in vertical:
        message.arrived()
    up_bl, up_br = positive(from_up[...]), positive(-from_up[...])
    down_tl, down_tr = positive(from_down[...]), positive(-from_down[...])
    column_top = jnp.concatenate([start[...], start_up[...]], axis=0)
    column_bottom = jnp.concatenate([start[...], start_down[...]], axis=0)
    stack_tl = jnp.concatenate([own_tl, up_bl], axis=0)
    stack_tr = jnp.concatenate([own_tr, up_br], axis=0)
    stack_bl = jnp.concatenate([own_bl, down_tl], axis=0)
    stack_br = jnp.concatenate([own_br, down_tr], axis=0)

    near_rows = (lax.broadcasted_iota(i32, (PIX, F), 0) & 31) < HALF

    def residual(pixels, near, stack, column):
        seen = pixels[...].reshape(PIX, F).astype(f32)
        seen = jnp.where(near_rows, seen, 0.0) if near else jnp.where(near_rows, 0.0, seen)
        rest = seen - tn(stack, column)
        high = rounded(rest)
        return jnp.concatenate([high, rest - high], axis=1).astype(bf16)

    rest_tl = residual(top_movie, True, stack_tl, column_top)
    rest_tr = residual(top_movie, False, stack_tr, column_top)
    rest_bl = residual(bottom_movie, True, stack_bl, column_bottom)
    rest_br = residual(bottom_movie, False, stack_br, column_bottom)
    both = nn(own_tl, rest_tl) + nn(own_tr, rest_tr) + nn(own_bl, rest_bl) + nn(own_br, rest_br)
    total = both[:, :F] + both[:, F:]

    def halves(rows):
        l, r = from_left[rows, :], from_right[rows, :]
        return positive(l), positive(-l), positive(r), positive(-r)

    def side_sums(l_tr, l_br, r_tl, r_bl):
        l = nn(l_tr, rest_tl) + nn(l_br, rest_bl)
        r = nn(r_tl, rest_tr) + nn(r_bl, rest_br)
        return l[:, :F] + l[:, F:], r[:, :F] + r[:, F:]

    def side_parts(q):
        for message in side[q]:
            message.arrived()
        parts = halves(slice(q * ROWS, (q + 1) * ROWS))
        return parts, side_sums(*parts)

    def to_band(i, q, l_sum, r_sum):
        about[i, 0], about[i, 1], about[i, 2] = l_sum, total[q * ROWS:(q + 1) * ROWS], r_sum
        messages = []
        for o in BAND:
            low, high = max(0, o[1]), min(3, 3 + o[1])
            messages.append(
                Remote(
                    about.at[i, pl.ds(low, high - low)],
                    abouts.at[i, 1 - o[0], 2 - o[1], pl.ds(low - o[1], high - low)], o,
                ).start()
            )
        return messages

    def give_back(i, l_sum, r_sum):
        sum_left[i], sum_right[i] = l_sum, r_sum
        return [
            Remote(sum_left.at[i], sum_from_right.at[i], LEFT).start(),
            Remote(sum_right.at[i], sum_from_left.at[i], RIGHT).start(),
        ]

    parts0, sums = side_parts(0)
    band = [to_band(0, 0, *sums)]
    parts1, sums = side_parts(1)
    returned = give_back(0, *sums)
    for message in side[3] + known[1]:
        message.start()
    parts2, sums = side_parts(2)
    band.append(to_band(1, 2, *sums))

    l_tr, l_br, r_tl, r_bl = (
        jnp.concatenate(x, axis=0) for x in zip(parts0, parts1, parts2)
    )
    gram_tl, gram_bl = nt(l_tr, stack_tl), nt(l_br, stack_bl)
    gram_tr, gram_br = nt(r_tl, stack_tr), nt(r_bl, stack_br)
    cross_up[...] = jnp.concatenate([gram_tl[:, K:], gram_tr[:, K:]], axis=0)
    cross_down[...] = jnp.concatenate([gram_bl[:, K:], gram_br[:, K:]], axis=0)
    crossing = [
        Remote(cross_up, cross_from_down, UP).start(),
        Remote(cross_down, cross_from_up, DOWN).start(),
    ]
    own_left = gram_tl[:, :K] + gram_bl[:, :K]
    own_right = gram_tr[:, :K] + gram_br[:, :K]
    own_top = nt(stack_tl, own_tl) + nt(stack_tr, own_tr)
    own_bottom = nt(stack_bl, own_bl) + nt(stack_br, own_br)
    own_own = own_top[:K] + own_bottom[:K]
    own_up, own_down = own_top[K:], own_bottom[K:]

    for message in crossing:
        message.arrived()
    around = [
        cross_from_up[:3 * ROWS, :], own_up, cross_from_up[3 * ROWS:, :],
        own_left, own_own, own_right,
        cross_from_down[:3 * ROWS, :], own_down, cross_from_down[3 * ROWS:, :],
    ]
    columns = [
        jnp.concatenate([m[q * ROWS:(q + 1) * ROWS] for m in around], axis=0).T
        for q in range(BLOCKS - 1)
    ]
    margin[...] = columns[1][2 * ROWS:3 * ROWS]
    lent = [Remote(margin, margins.at[slot(flip(o))], o).start() for o in NEAR if o != HERE]
    columns = [lanes_of(x) for x in columns]

    def stepped(previous, left_over, level):
        return jnp.maximum(previous + left_over / level, 0.0)

    def rows(q):
        return slice(q * ROWS, (q + 1) * ROWS)

    def facts(i, q):
        for message in known[i]:
            message.arrived()
        found = {HERE: (start_value[rows(q)], divisor[rows(q)])}
        for o in NEAR:
            if o != HERE:
                x = infos[i, slot(o)].astype(f32)
                level = x[ROWS:, 0:1] + x[ROWS:, 1:2] + x[ROWS:, 2:3]
                found[o] = (x[:ROWS], jnp.where(level == 0.0, 1.0, level))
        return found

    def band_sum(i, o):
        left_over = None
        for v in range(-2, 3):
            if abs(v - o[1]) > 1:
                continue
            piece = (
                about[i, o[1] + 1] if (o[0], v) == HERE
                else abouts[i, o[0] + 1, v + 2, o[1] + 1]
            )
            left_over = piece if left_over is None else left_over + piece
        return left_over

    known_now = facts(0, 0)
    for message in band[0]:
        message.arrived()
    moved = []
    for o in NEAR:
        previous, level = known_now[o]
        renewed = stepped(previous, band_sum(0, o), level)
        if o == HERE:
            renewed = jnp.where(alive_col[rows(0)], renewed, 0.0)
            current = [renewed]
        moved.append(renewed - previous)
    change = nn(columns[0][ROWS:], rows_of(jnp.concatenate(moved, axis=0)))

    for message in returned:
        message.arrived()
    left_over = total[rows(1)] + sum_from_left[0] + sum_from_right[0] - change[:ROWS]
    previous = start_value[rows(1)]
    renewed = stepped(previous, left_over, divisor[rows(1)])
    renewed = jnp.where(alive_col[rows(1)], renewed, 0.0)
    current.append(renewed)
    own_step = renewed - previous
    step[:ROWS, :] = own_step
    step[ROWS:, :] = change[ROWS:2 * ROWS]
    moves = [
        Remote(step, steps.at[slot(flip(o))], o).start() if o in NEAR
        else Remote(
            step.at[pl.ds(0, ROWS)], far_steps.at[RING.index(flip(o))], o
        ).start()
        for o in OUTWARD
    ]
    _, sums = side_parts(3)
    returned_late = give_back(1, *sums)
    known_now = facts(1, 2)
    for message in band[1]:
        message.arrived()
    for message in lent:
        message.arrived()
    weights = {
        o: lanes_of(margin[...] if o == HERE else margins[slot(o)]) for o in NEAR
    }

    for message in moves:
        message.arrived()
    taken = {
        o: own_step if o == HERE
        else steps[slot(o), :ROWS, :] if o in NEAR
        else far_steps[RING.index(o)]
        for o in WIDE
    }
    moved = []
    for o in NEAR:
        nearby = rows_of(jnp.concatenate([taken[plus(o, p)] for p in NEAR], axis=0))
        if o == HERE:
            left_over = band_sum(1, o) - change[ROWS:2 * ROWS]
            last_change = change[2 * ROWS:] + nn(columns[1][3 * ROWS:], nearby)
        else:
            left_over = band_sum(1, o) - steps[slot(o), ROWS:, :]
        left_over = left_over - nn(weights[o], nearby)
        previous, level = known_now[o]
        renewed = stepped(previous, left_over, level)
        if o == HERE:
            renewed = jnp.where(alive_col[rows(2)], renewed, 0.0)
            current.append(renewed)
        moved.append(renewed - previous)

    last_change = last_change + nn(
        columns[2][3 * ROWS:], rows_of(jnp.concatenate(moved, axis=0))
    )
    for message in returned_late:
        message.arrived()
    last = total[rows(3)] + sum_from_left[1] + sum_from_right[1] - last_change
    renewed = stepped(start_value[rows(3)], last, divisor[rows(3)])
    current.append(jnp.where(alive_col[rows(3)], renewed, 0.0))
    result = jnp.concatenate(current, axis=0)
    high = rounded(result)
    mid = rounded(result - high)
    back = jnp.where(sub == order_row, 1.0, 0.0)
    out[...] = nn(
        jnp.concatenate([back, back, back], axis=1).astype(bf16),
        jnp.concatenate([high, mid, result - high - mid], axis=0).astype(bf16),
    )
    for message in sent:
        message.left()


def body(movie, footprints, centres, traces, counts, order):
    messages = 8 + 6 + 16 + 2 * len(BAND) + 4 + 2 + 8 + 24
    any_space = pl.BlockSpec(memory_space=pl.ANY)
    result = pl.pallas_call(
        kernel,
        name="hals",
        out_shape=pltpu.VMEM((K, F), f32),
        in_specs=[any_space] * 6,
        out_specs=pl.BlockSpec(memory_space=pltpu.VMEM),
        scratch_shapes=[
            pltpu.VMEM((K, PIX), bf16), pltpu.VMEM((2, K), i32), pltpu.VMEM((K, F), bf16),
            pltpu.VMEM((1, 1), i32), pltpu.VMEM((1, K), i32),
            pltpu.VMEM((SIDE, SIDE, F), bf16), pltpu.VMEM((SIDE, SIDE, F), bf16),
            *[pltpu.VMEM((K, PIX), bf16) for _ in range(8)],
            *[pltpu.VMEM((K, F), bf16) for _ in range(3)],
            pltpu.VMEM((2, 2 * ROWS, F), bf16), pltpu.VMEM((2, 9, 2 * ROWS, F), bf16),
            pltpu.VMEM((2, 3, ROWS, F), f32), pltpu.VMEM((2, 3, 5, 3, ROWS, F), f32),
            *[pltpu.VMEM((2, ROWS, F), f32) for _ in range(4)],
            *[pltpu.VMEM((6 * ROWS, K), f32) for _ in range(4)],
            pltpu.VMEM((ROWS, 9 * ROWS), f32), pltpu.VMEM((9, ROWS, 9 * ROWS), f32),
            pltpu.VMEM((2 * ROWS, F), f32), pltpu.VMEM((9, 2 * ROWS, F), f32),
            pltpu.VMEM((len(RING), ROWS, F), f32),
            pltpu.SemaphoreType.DMA((7,)),
            pltpu.SemaphoreType.DMA((messages,)), pltpu.SemaphoreType.DMA((messages,)),
        ],
        compiler_params=pltpu.CompilerParams(collective_id=0, has_side_effects=True),
    )(movie, footprints[0, 0], centres[0, 0].T, traces[0, 0], counts, order[0])
    return result[None, None]


def solution(mesh):
    in_specs = (
        P("ty", "tx", None),
        P("ty", "tx", None, None),
        P("ty", "tx", None, None),
        P("ty", "tx", None, None),
        P("ty", "tx"),
        P("ty", "tx", None),
    )
    out_specs = P("ty", "tx", None, None)
    return jax.shard_map(body, mesh=mesh, in_specs=in_specs, out_specs=out_specs, check_vma=False)
```

```python
import jax
import jax.numpy as jnp
from jax import lax
from jax.experimental import pallas as pl
from jax.experimental.pallas import tpu as pltpu
from jax.sharding import PartitionSpec as P

K = 32
F = 128
SIDE = 32
PIX = SIDE * SIDE
HALF = SIDE // 2
ROWS = 8
BLOCKS = 4
MESH = pl.DeviceIdType.MESH
NEAR = [(u, v) for u in (-1, 0, 1) for v in (-1, 0, 1)]
WIDE = [(u, v) for u in range(-2, 3) for v in range(-2, 3)]
RING = [o for o in WIDE if o not in NEAR]
BAND = [(u, v) for v in (-1, 1, -2, 2, 0) for u in (0, -1, 1) if (u, v) != (0, 0)]
OUTWARD = [(u, v) for v in (-1, 1, -2, 2, 0) for u in (0, -1, 1, -2, 2) if (u, v) != (0, 0)]
HERE = (0, 0)
f32, bf16, i32 = jnp.float32, jnp.bfloat16, jnp.int32
UP, DOWN, LEFT, RIGHT = (-1, 0), (1, 0), (0, -1), (0, 1)


def flip(o):
    return (-o[0], -o[1])


def plus(o, p):
    return (o[0] + p[0], o[1] + p[1])


def nt(x, y):
    return lax.dot_general(x, y, (((1,), (1,)), ((), ())), preferred_element_type=f32)


def tn(x, y):
    return lax.dot_general(x, y, (((0,), (0,)), ((), ())), preferred_element_type=f32)


def nn(x, y):
    return jnp.dot(x, y, preferred_element_type=f32)


def rounded(x):
    return x.astype(bf16).astype(f32)


def lanes_of(x):
    high = rounded(x)
    return jnp.concatenate([high, high, x - high], axis=1).astype(bf16)


def rows_of(x):
    high = rounded(x)
    return jnp.concatenate([high, x - high, high], axis=0).astype(bf16)


def positive(x):
    return jnp.maximum(x, jnp.zeros_like(x))


def kernel(
    movie, foot_in, centres_in, traces_in, counts_in, order_in, out,
    foot, centres, traces, counts, order,
    top_movie, bottom_movie, to_left, to_right, to_up, to_down,
    from_right, from_left, from_down, from_up,
    start, start_up, start_down, infos,
    about, abouts, sum_left, sum_right, sum_from_right, sum_from_left,
    cross_up, cross_down, cross_from_down, cross_from_up,
    margins, step, steps, far_steps,
    local_sem, send_sem, recv_sem,
):
    a, b = lax.axis_index("ty"), lax.axis_index("tx")
    n_ty, n_tx = lax.axis_size("ty"), lax.axis_size("tx")

    def there(o):
        row, col = a + o[0], b + o[1]
        return (row >= 0) & (row < n_ty) & (col >= 0) & (col < n_tx)

    barrier = pltpu.get_barrier_semaphore()
    expected = jnp.int32(0)
    for o in NEAR:
        if o == HERE:
            continue
        present = there(o)

        @pl.when(present)
        def _(o=o):
            pl.semaphore_signal(
                barrier, inc=1, device_id=(a + o[0], b + o[1]), device_id_type=MESH
            )

        expected = expected + present.astype(i32)

    local = []
    for source, target in (
        (order_in, order), (counts_in, counts), (centres_in, centres), (foot_in, foot),
        (traces_in, traces), (movie.at[pl.ds(0, HALF)], top_movie.at[pl.ds(0, HALF)]),
        (movie.at[pl.ds(HALF, HALF)], bottom_movie.at[pl.ds(HALF, HALF)]),
    ):
        copy = pltpu.make_async_copy(source, target, local_sem.at[len(local)])
        copy.start()
        local.append(copy)

    sent = []

    class Remote:
        def __init__(self, source, target, o):
            self.o = o
            index = len(sent)
            self.copy = pltpu.make_async_remote_copy(
                src_ref=source, dst_ref=target,
                send_sem=send_sem.at[index], recv_sem=recv_sem.at[index],
                device_id=(a + o[0], b + o[1]), device_id_type=MESH,
            )
            sent.append(self)

        def start(self):
            pl.when(there(self.o))(self.copy.start)
            return self

        def arrived(self):
            pl.when(there(flip(self.o)))(self.copy.wait_recv)

        def left(self):
            pl.when(there(self.o))(self.copy.wait_send)

    def clear(o, *refs):
        @pl.when(jnp.logical_not(there(o)))
        def _():
            for ref in refs:
                ref[...] = jnp.zeros_like(ref)

    def slot(o):
        return (o[0] + 1) * 3 + o[1] + 1

    clear(UP, from_up, start_up, cross_from_up, top_movie.at[pl.ds(HALF, HALF)])
    clear(DOWN, from_down, start_down, cross_from_down, bottom_movie.at[pl.ds(0, HALF)])
    clear(LEFT, from_left, sum_from_left)
    clear(RIGHT, from_right, sum_from_right)
    for o in NEAR:
        if o != HERE:
            clear(o, steps.at[slot(o)])
    for o in (UP, DOWN):
        clear(o, infos.at[o[0] + 1], margins.at[o[0] + 1])
    for o in (LEFT, RIGHT):
        clear(o, infos.at[1, o[1] + 1], margins.at[1, o[1] + 1])
    for o in BAND:
        clear(o, abouts.at[o[0] + 1, o[1] + 2])
    for o in RING:
        clear(o, far_steps.at[RING.index(o)])

    for copy in local[:3]:
        copy.wait()
    sub = lax.broadcasted_iota(i32, (K, K), 0)
    lane = lax.broadcasted_iota(i32, (K, K), 1)

    def to_column(row, pick):
        spread = jnp.where(pick, jnp.broadcast_to(row, (K, K)), 0)
        return jnp.sum(spread.astype(f32), axis=1, keepdims=True)

    order_row = order[0:1, :]
    order_col = to_column(order_row, sub == lane).astype(i32)
    alive_col = order_col < counts[0:1, 0:1]
    picked = (lane == order_col) & alive_col
    row_at = to_column(centres[0:1, :], picked).astype(i32)
    col_at = to_column(centres[1:2, :], picked).astype(i32)
    for copy in local[3:5]:
        copy.wait()
    chooser = jnp.where(picked, 1.0, 0.0).astype(bf16)
    ordered = nn(chooser, foot[...])
    start_value = nn(chooser, traces[...])
    start[...] = start_value.astype(bf16)
    diagonal = jnp.sum(ordered * ordered, axis=1, keepdims=True)
    divisor = jnp.where(alive_col, diagonal, 1.0)
    level = jnp.broadcast_to(divisor, (K, F))
    level_high = rounded(level)
    level_mid = rounded(level - level_high)
    level_low = level - level_high - level_mid
    wide_lane = lax.broadcasted_iota(i32, (K, F), 1)
    level_parts = jnp.where(
        wide_lane == 0, level_high, jnp.where(wide_lane == 1, level_mid, level_low)
    )
    for i, q in enumerate((0, 2)):
        infos[1, 1, i] = jnp.concatenate(
            [x[q * ROWS:(q + 1) * ROWS] for x in (start_value, level_parts)], axis=0
        ).astype(bf16)

    group, across = wide_lane >> 5, wide_lane & 31
    turn, shift = (row_at + HALF) & 31, (col_at + HALF) & 31
    fine, coarse = turn & 3, turn >> 2
    index = (((group - fine) & 3) << 5) + ((across - shift) & 31)
    slabs = [
        jnp.take_along_axis(ordered[:, v * F:(v + 1) * F], index, axis=1) for v in range(8)
    ]
    carry = group < fine
    slabs = [jnp.where(carry, slabs[(v - 1) % 8], slabs[v]) for v in range(8)]
    for bit in (1, 2, 4):
        taken = jnp.broadcast_to((coarse & bit) != 0, (K, F))
        slabs = [jnp.where(taken, slabs[(v - bit) % 8], slabs[v]) for v in range(8)]
    left_half = ((across + HALF) & 31) >= col_at
    for v in range(8):
        upper = ((4 * v + group + HALF) & 31) >= row_at
        x = slabs[v]
        by_row = jnp.where(upper, x, -x)
        by_col = jnp.where(left_half, x, -x)
        here = pl.ds(v * F, F)
        to_left[:, here] = jnp.where(left_half, by_row, 0.0).astype(bf16)
        to_right[:, here] = jnp.where(left_half, 0.0, by_row).astype(bf16)
        to_up[:, here] = jnp.where(upper, by_col, 0.0).astype(bf16)
        to_down[:, here] = jnp.where(upper, 0.0, by_col).astype(bf16)
    for copy in local[5:]:
        copy.wait()

    pl.semaphore_wait(barrier, expected)

    def chunk(q):
        return pl.ds(q * ROWS, ROWS)

    side = [
        [Remote(to_left.at[chunk(q)], from_right.at[chunk(q)], LEFT),
         Remote(to_right.at[chunk(q)], from_left.at[chunk(q)], RIGHT)]
        for q in range(BLOCKS)
    ]
    vertical = [
        Remote(to_up, from_down, UP), Remote(to_down, from_up, DOWN),
        Remote(start, start_down, UP), Remote(start, start_up, DOWN),
        Remote(top_movie.at[pl.ds(0, HALF)], bottom_movie.at[pl.ds(0, HALF)], UP),
        Remote(bottom_movie.at[pl.ds(HALF, HALF)], top_movie.at[pl.ds(HALF, HALF)], DOWN),
    ]
    def along(ref):
        return [Remote(ref.at[1, 1], ref.at[1, 1 - o[1]], o).start() for o in (LEFT, RIGHT)]

    def across(ref, messages):
        for message in messages:
            message.arrived()
        return [Remote(ref.at[1], ref.at[1 - o[0]], o).start() for o in (UP, DOWN)]

    for message in side[0] + vertical + side[1] + side[2]:
        message.start()
    known = along(infos)

    own_tl, own_bl = positive(to_left[...]), positive(-to_left[...])
    own_tr, own_br = positive(to_right[...]), positive(-to_right[...])
    for message in vertical:
        message.arrived()
    up_bl, up_br = positive(from_up[...]), positive(-from_up[...])
    down_tl, down_tr = positive(from_down[...]), positive(-from_down[...])
    column_top = jnp.concatenate([start[...], start_up[...]], axis=0)
    column_bottom = jnp.concatenate([start[...], start_down[...]], axis=0)
    stack_tl = jnp.concatenate([own_tl, up_bl], axis=0)
    stack_tr = jnp.concatenate([own_tr, up_br], axis=0)
    stack_bl = jnp.concatenate([own_bl, down_tl], axis=0)
    stack_br = jnp.concatenate([own_br, down_tr], axis=0)

    near_rows = (lax.broadcasted_iota(i32, (PIX, F), 0) & 31) < HALF

    def residual(pixels, near, stack, column):
        seen = pixels[...].reshape(PIX, F).astype(f32)
        seen = jnp.where(near_rows, seen, 0.0) if near else jnp.where(near_rows, 0.0, seen)
        rest = seen - tn(stack, column)
        high = rounded(rest)
        return jnp.concatenate([high, rest - high], axis=1).astype(bf16)

    rest_tl = residual(top_movie, True, stack_tl, column_top)
    rest_tr = residual(top_movie, False, stack_tr, column_top)
    rest_bl = residual(bottom_movie, True, stack_bl, column_bottom)
    rest_br = residual(bottom_movie, False, stack_br, column_bottom)
    both = nn(own_tl, rest_tl) + nn(own_tr, rest_tr) + nn(own_bl, rest_bl) + nn(own_br, rest_br)
    total = both[:, :F] + both[:, F:]

    def halves(rows):
        l, r = from_left[rows, :], from_right[rows, :]
        return positive(l), positive(-l), positive(r), positive(-r)

    def side_sums(l_tr, l_br, r_tl, r_bl):
        l = nn(l_tr, rest_tl) + nn(l_br, rest_bl)
        r = nn(r_tl, rest_tr) + nn(r_bl, rest_br)
        return l[:, :F] + l[:, F:], r[:, :F] + r[:, F:]

    def side_parts(q):
        for message in side[q]:
            message.arrived()
        parts = halves(slice(q * ROWS, (q + 1) * ROWS))
        return parts, side_sums(*parts)

    def to_band(l_sum, r_sum):
        about[0], about[1], about[2] = l_sum, total[:ROWS], r_sum
        messages = []
        for o in BAND:
            low, high = max(0, o[1]), min(3, 3 + o[1])
            messages.append(
                Remote(
                    about.at[pl.ds(low, high - low)],
                    abouts.at[1 - o[0], 2 - o[1], pl.ds(low - o[1], high - low)], o,
                ).start()
            )
        return messages

    def give_back(i, l_sum, r_sum):
        sum_left[i], sum_right[i] = l_sum, r_sum
        return [
            Remote(sum_left.at[i], sum_from_right.at[i], LEFT).start(),
            Remote(sum_right.at[i], sum_from_left.at[i], RIGHT).start(),
        ]

    def meet(q, l_tr, l_br, r_tl, r_bl):
        gram_tl, gram_bl = nt(l_tr, stack_tl), nt(l_br, stack_bl)
        gram_tr, gram_br = nt(r_tl, stack_tr), nt(r_bl, stack_br)
        cross_up[q] = jnp.concatenate([gram_tl[:, K:], gram_tr[:, K:]], axis=0)
        cross_down[q] = jnp.concatenate([gram_bl[:, K:], gram_br[:, K:]], axis=0)
        crossing = [
            Remote(cross_up.at[q], cross_from_down.at[q], UP).start(),
            Remote(cross_down.at[q], cross_from_up.at[q], DOWN).start(),
        ]
        return crossing, gram_tl[:, :K] + gram_bl[:, :K], gram_tr[:, :K] + gram_br[:, :K]

    met, returned = [], []
    for q in range(BLOCKS - 1):
        parts, sums = side_parts(q)
        if q == 0:
            band = to_band(*sums)
        else:
            returned += give_back(q - 1, *sums)
        met.append(meet(q, *parts))
    for message in side[3]:
        message.start()
    own_top = nt(stack_tl, own_tl) + nt(stack_tr, own_tr)
    own_bottom = nt(stack_bl, own_bl) + nt(stack_br, own_br)
    own_own = own_top[:K] + own_bottom[:K]
    own_up, own_down = own_top[K:], own_bottom[K:]

    def column(q):
        crossing, own_left, own_right = met[q]
        for message in crossing:
            message.arrived()
        mine = slice(q * ROWS, (q + 1) * ROWS)
        above, below = cross_from_up[q], cross_from_down[q]
        return jnp.concatenate(
            [above[:ROWS], own_up[mine], above[ROWS:], own_left, own_own[mine], own_right,
             below[:ROWS], own_down[mine], below[ROWS:]], axis=0
        ).T

    columns = [None] * (BLOCKS - 1)
    known = across(infos, known)
    columns[1] = column(1)
    margins[1, 1] = columns[1][2 * ROWS:3 * ROWS]
    lent = along(margins)
    columns[1] = lanes_of(columns[1])
    columns[0] = lanes_of(column(0))

    def stepped(previous, left_over, level):
        return jnp.maximum(previous + left_over / level, 0.0)

    def rows(q):
        return slice(q * ROWS, (q + 1) * ROWS)

    def facts(i, q):
        found = {HERE: (start_value[rows(q)], divisor[rows(q)])}
        for o in NEAR:
            if o != HERE:
                x = infos[o[0] + 1, o[1] + 1, i].astype(f32)
                level = x[ROWS:, 0:1] + x[ROWS:, 1:2] + x[ROWS:, 2:3]
                found[o] = (x[:ROWS], jnp.where(level == 0.0, 1.0, level))
        return found

    def band_sum(o):
        left_over = None
        for v in range(-2, 3):
            if abs(v - o[1]) > 1:
                continue
            piece = (
                about[o[1] + 1] if (o[0], v) == HERE
                else abouts[o[0] + 1, v + 2, o[1] + 1]
            )
            left_over = piece if left_over is None else left_over + piece
        return left_over

    for message in known:
        message.arrived()
    known_now = facts(0, 0)
    for message in band:
        message.arrived()
    moved = []
    for o in NEAR:
        previous, level = known_now[o]
        renewed = stepped(previous, band_sum(o), level)
        if o == HERE:
            renewed = jnp.where(alive_col[rows(0)], renewed, 0.0)
            current = [renewed]
        moved.append(renewed - previous)
    change = nn(columns[0][ROWS:], rows_of(jnp.concatenate(moved, axis=0)))

    for message in returned:
        message.arrived()
    left_over = total[rows(1)] + sum_from_left[0] + sum_from_right[0] - change[:ROWS]
    previous = start_value[rows(1)]
    renewed = stepped(previous, left_over, divisor[rows(1)])
    renewed = jnp.where(alive_col[rows(1)], renewed, 0.0)
    current.append(renewed)
    own_step = renewed - previous
    step[:ROWS, :] = own_step
    own_sum = total[rows(2)] + sum_from_left[1] + sum_from_right[1] - change[ROWS:2 * ROWS]
    step[ROWS:, :] = own_sum
    moves = [
        Remote(step, steps.at[slot(flip(o))], o).start() if o in NEAR
        else Remote(
            step.at[pl.ds(0, ROWS)], far_steps.at[RING.index(flip(o))], o
        ).start()
        for o in OUTWARD
    ]
    lent = across(margins, lent)
    _, sums = side_parts(3)
    returned_late = give_back(2, *sums)
    columns[2] = lanes_of(column(2))
    known_now = facts(1, 2)
    for message in lent:
        message.arrived()
    weights = {
        o: lanes_of(margins[o[0] + 1, o[1] + 1]) for o in NEAR
    }

    for message in moves:
        message.arrived()
    taken = {
        o: own_step if o == HERE
        else steps[slot(o), :ROWS, :] if o in NEAR
        else far_steps[RING.index(o)]
        for o in WIDE
    }
    moved = []
    for o in NEAR:
        nearby = rows_of(jnp.concatenate([taken[plus(o, p)] for p in NEAR], axis=0))
        if o == HERE:
            left_over = own_sum
            last_change = change[2 * ROWS:] + nn(columns[1][3 * ROWS:], nearby)
        else:
            left_over = steps[slot(o), ROWS:, :]
        left_over = left_over - nn(weights[o], nearby)
        previous, level = known_now[o]
        renewed = stepped(previous, left_over, level)
        if o == HERE:
            renewed = jnp.where(alive_col[rows(2)], renewed, 0.0)
            current.append(renewed)
        moved.append(renewed - previous)

    last_change = last_change + nn(
        columns[2][3 * ROWS:], rows_of(jnp.concatenate(moved, axis=0))
    )
    for message in returned_late:
        message.arrived()
    last = total[rows(3)] + sum_from_left[2] + sum_from_right[2] - last_change
    renewed = stepped(start_value[rows(3)], last, divisor[rows(3)])
    current.append(jnp.where(alive_col[rows(3)], renewed, 0.0))
    result = jnp.concatenate(current, axis=0)
    high = rounded(result)
    mid = rounded(result - high)
    back = jnp.where(sub == order_row, 1.0, 0.0)
    out[...] = nn(
        jnp.concatenate([back, back, back], axis=1).astype(bf16),
        jnp.concatenate([high, mid, result - high - mid], axis=0).astype(bf16),
    )
    for message in sent:
        message.left()


def body(movie, footprints, centres, traces, counts, order):
    messages = 8 + 6 + 4 + len(BAND) + 6 + 6 + 4 + 24
    any_space = pl.BlockSpec(memory_space=pl.ANY)
    result = pl.pallas_call(
        kernel,
        name="hals",
        out_shape=pltpu.VMEM((K, F), f32),
        in_specs=[any_space] * 6,
        out_specs=pl.BlockSpec(memory_space=pltpu.VMEM),
        scratch_shapes=[
            pltpu.VMEM((K, PIX), bf16), pltpu.VMEM((2, K), i32), pltpu.VMEM((K, F), bf16),
            pltpu.VMEM((1, 1), i32), pltpu.VMEM((1, K), i32),
            pltpu.VMEM((SIDE, SIDE, F), bf16), pltpu.VMEM((SIDE, SIDE, F), bf16),
            *[pltpu.VMEM((K, PIX), bf16) for _ in range(8)],
            *[pltpu.VMEM((K, F), bf16) for _ in range(3)],
            pltpu.VMEM((3, 3, 2, 2 * ROWS, F), bf16),
            pltpu.VMEM((3, ROWS, F), f32), pltpu.VMEM((3, 5, 3, ROWS, F), f32),
            *[pltpu.VMEM((3, ROWS, F), f32) for _ in range(4)],
            *[pltpu.VMEM((3, 2 * ROWS, K), f32) for _ in range(4)],
            pltpu.VMEM((3, 3, ROWS, 9 * ROWS), f32),
            pltpu.VMEM((2 * ROWS, F), f32), pltpu.VMEM((9, 2 * ROWS, F), f32),
            pltpu.VMEM((len(RING), ROWS, F), f32),
            pltpu.SemaphoreType.DMA((7,)),
            pltpu.SemaphoreType.DMA((messages,)), pltpu.SemaphoreType.DMA((messages,)),
        ],
        compiler_params=pltpu.CompilerParams(collective_id=0, has_side_effects=True),
    )(movie, footprints[0, 0], centres[0, 0].T, traces[0, 0], counts, order[0])
    return result[None, None]


def solution(mesh):
    in_specs = (
        P("ty", "tx", None),
        P("ty", "tx", None, None),
        P("ty", "tx", None, None),
        P("ty", "tx", None, None),
        P("ty", "tx"),
        P("ty", "tx", None),
    )
    out_specs = P("ty", "tx", None, None)
    return jax.shard_map(body, mesh=mesh, in_specs=in_specs, out_specs=out_specs, check_vma=False)
```

```python
import jax
import jax.numpy as jnp
from jax import lax
from jax.experimental import pallas as pl
from jax.experimental.pallas import tpu as pltpu
from jax.sharding import PartitionSpec as P

K = 32
F = 128
SIDE = 32
PIX = SIDE * SIDE
HALF = SIDE // 2
ROWS = 8
BLOCKS = 4
MESH = pl.DeviceIdType.MESH
NEAR = [(u, v) for u in (-1, 0, 1) for v in (-1, 0, 1)]
WIDE = [(u, v) for u in range(-2, 3) for v in range(-2, 3)]
RING = [o for o in WIDE if o not in NEAR]
BAND = [(u, v) for v in (-1, 1, -2, 2, 0) for u in (0, -1, 1) if (u, v) != (0, 0)]
OUTWARD = [(u, v) for v in (-1, 1, -2, 2, 0) for u in (0, -1, 1, -2, 2) if (u, v) != (0, 0)]
HERE = (0, 0)
f32, bf16, i32 = jnp.float32, jnp.bfloat16, jnp.int32
UP, DOWN, LEFT, RIGHT = (-1, 0), (1, 0), (0, -1), (0, 1)


def flip(o):
    return (-o[0], -o[1])


def plus(o, p):
    return (o[0] + p[0], o[1] + p[1])


def nt(x, y):
    return lax.dot_general(x, y, (((1,), (1,)), ((), ())), preferred_element_type=f32)


def tn(x, y):
    return lax.dot_general(x, y, (((0,), (0,)), ((), ())), preferred_element_type=f32)


def nn(x, y):
    return jnp.dot(x, y, preferred_element_type=f32)


def rounded(x):
    return x.astype(bf16).astype(f32)


def lanes_of(x):
    high = rounded(x)
    return jnp.concatenate([high, high, x - high], axis=1).astype(bf16)


def rows_of(x):
    high = rounded(x)
    return jnp.concatenate([high, x - high, high], axis=0).astype(bf16)


def positive(x):
    return jnp.maximum(x, jnp.zeros_like(x))


def kernel(
    movie, foot_in, centres_in, traces_in, counts_in, order_in, out,
    foot, centres, traces, counts, order,
    top_movie, bottom_movie, to_left, to_right, to_up, to_down,
    from_right, from_left, from_down, from_up,
    start, start_up, start_down, infos,
    about, abouts, sum_left, sum_right, sum_from_right, sum_from_left,
    cross_up, cross_down, cross_from_down, cross_from_up,
    margins, step, steps, far_steps, left_sum, left_sums, recon,
    local_sem, send_sem, recv_sem,
):
    a, b = lax.axis_index("ty"), lax.axis_index("tx")
    n_ty, n_tx = lax.axis_size("ty"), lax.axis_size("tx")

    def there(o):
        row, col = a + o[0], b + o[1]
        return (row >= 0) & (row < n_ty) & (col >= 0) & (col < n_tx)

    barrier = pltpu.get_barrier_semaphore()
    expected = jnp.int32(0)
    for o in NEAR:
        if o == HERE:
            continue
        present = there(o)

        @pl.when(present)
        def _(o=o):
            pl.semaphore_signal(
                barrier, inc=1, device_id=(a + o[0], b + o[1]), device_id_type=MESH
            )

        expected = expected + present.astype(i32)

    local = []
    for source, target in (
        (order_in, order), (counts_in, counts), (centres_in, centres), (foot_in, foot),
        (traces_in, traces), (movie.at[pl.ds(0, HALF)], top_movie.at[pl.ds(0, HALF)]),
        (movie.at[pl.ds(HALF, HALF)], bottom_movie.at[pl.ds(HALF, HALF)]),
    ):
        copy = pltpu.make_async_copy(source, target, local_sem.at[len(local)])
        copy.start()
        local.append(copy)

    sent = []

    class Remote:
        def __init__(self, source, target, o):
            self.o = o
            index = len(sent)
            self.copy = pltpu.make_async_remote_copy(
                src_ref=source, dst_ref=target,
                send_sem=send_sem.at[index], recv_sem=recv_sem.at[index],
                device_id=(a + o[0], b + o[1]), device_id_type=MESH,
            )
            sent.append(self)

        def start(self):
            pl.when(there(self.o))(self.copy.start)
            return self

        def arrived(self):
            pl.when(there(flip(self.o)))(self.copy.wait_recv)

        def left(self):
            pl.when(there(self.o))(self.copy.wait_send)

    def clear(o, *refs):
        @pl.when(jnp.logical_not(there(o)))
        def _():
            for ref in refs:
                ref[...] = jnp.zeros_like(ref)

    def slot(o):
        return (o[0] + 1) * 3 + o[1] + 1

    clear(UP, from_up, start_up, cross_from_up, top_movie.at[pl.ds(HALF, HALF)])
    clear(DOWN, from_down, start_down, cross_from_down, bottom_movie.at[pl.ds(0, HALF)])
    clear(LEFT, from_left, sum_from_left)
    clear(RIGHT, from_right, sum_from_right)
    for o in NEAR:
        if o != HERE:
            clear(o, steps.at[slot(o)], left_sums.at[slot(o)])
    for o in (UP, DOWN):
        clear(o, infos.at[0, o[0] + 1], infos.at[1, o[0] + 1], margins.at[o[0] + 1])
    for o in (LEFT, RIGHT):
        clear(o, infos.at[0, 1, o[1] + 1], infos.at[1, 1, o[1] + 1])
        clear(o, margins.at[1, o[1] + 1])
    for o in BAND:
        clear(o, abouts.at[o[0] + 1, o[1] + 2])
    for o in RING:
        clear(o, far_steps.at[RING.index(o)])

    for copy in local[:3]:
        copy.wait()
    sub = lax.broadcasted_iota(i32, (K, K), 0)
    lane = lax.broadcasted_iota(i32, (K, K), 1)

    def to_column(row, pick):
        spread = jnp.where(pick, jnp.broadcast_to(row, (K, K)), 0)
        return jnp.sum(spread.astype(f32), axis=1, keepdims=True)

    order_row = order[0:1, :]
    order_col = to_column(order_row, sub == lane).astype(i32)
    alive_col = order_col < counts[0:1, 0:1]
    picked = (lane == order_col) & alive_col
    row_at = to_column(centres[0:1, :], picked).astype(i32)
    col_at = to_column(centres[1:2, :], picked).astype(i32)
    for copy in local[3:5]:
        copy.wait()
    chooser = jnp.where(picked, 1.0, 0.0).astype(bf16)
    ordered = nn(chooser, foot[...])
    start_value = nn(chooser, traces[...])
    start[...] = start_value.astype(bf16)
    diagonal = jnp.sum(ordered * ordered, axis=1, keepdims=True)
    divisor = jnp.where(alive_col, diagonal, 1.0)
    level = jnp.broadcast_to(divisor, (K, F))
    level_high = rounded(level)
    level_mid = rounded(level - level_high)
    level_low = level - level_high - level_mid
    wide_lane = lax.broadcasted_iota(i32, (K, F), 1)
    level_parts = jnp.where(
        wide_lane == 0, level_high, jnp.where(wide_lane == 1, level_mid, level_low)
    )
    for i, q in enumerate((0, 2)):
        infos[i, 1, 1] = jnp.concatenate(
            [x[q * ROWS:(q + 1) * ROWS] for x in (start_value, level_parts)], axis=0
        ).astype(bf16)

    group, across = wide_lane >> 5, wide_lane & 31
    turn, shift = (row_at + HALF) & 31, (col_at + HALF) & 31
    fine, coarse = turn & 3, turn >> 2
    index = (((group - fine) & 3) << 5) + ((across - shift) & 31)
    slabs = [
        jnp.take_along_axis(ordered[:, v * F:(v + 1) * F], index, axis=1) for v in range(8)
    ]
    carry = group < fine
    slabs = [jnp.where(carry, slabs[(v - 1) % 8], slabs[v]) for v in range(8)]
    for bit in (1, 2, 4):
        taken = jnp.broadcast_to((coarse & bit) != 0, (K, F))
        slabs = [jnp.where(taken, slabs[(v - bit) % 8], slabs[v]) for v in range(8)]
    left_half = ((across + HALF) & 31) >= col_at
    for v in range(8):
        upper = ((4 * v + group + HALF) & 31) >= row_at
        x = slabs[v]
        by_row = jnp.where(upper, x, -x)
        by_col = jnp.where(left_half, x, -x)
        here = pl.ds(v * F, F)
        to_left[:, here] = jnp.where(left_half, by_row, 0.0).astype(bf16)
        to_right[:, here] = jnp.where(left_half, 0.0, by_row).astype(bf16)
        to_up[:, here] = jnp.where(upper, by_col, 0.0).astype(bf16)
        to_down[:, here] = jnp.where(upper, 0.0, by_col).astype(bf16)
    for copy in local[5:]:
        copy.wait()

    pl.semaphore_wait(barrier, expected)

    def chunk(q):
        return pl.ds(q * ROWS, ROWS)

    side = [
        [Remote(to_left.at[chunk(q)], from_right.at[chunk(q)], LEFT),
         Remote(to_right.at[chunk(q)], from_left.at[chunk(q)], RIGHT)]
        for q in range(BLOCKS)
    ]
    vertical = [
        Remote(to_up, from_down, UP), Remote(to_down, from_up, DOWN),
        Remote(start, start_down, UP), Remote(start, start_up, DOWN),
        Remote(top_movie.at[pl.ds(0, HALF)], bottom_movie.at[pl.ds(0, HALF)], UP),
        Remote(bottom_movie.at[pl.ds(HALF, HALF)], top_movie.at[pl.ds(HALF, HALF)], DOWN),
    ]
    def along(ref):
        return [Remote(ref.at[1, 1], ref.at[1, 1 - o[1]], o).start() for o in (LEFT, RIGHT)]

    def across(ref, messages):
        for message in messages:
            message.arrived()
        return [Remote(ref.at[1], ref.at[1 - o[0]], o).start() for o in (UP, DOWN)]

    for message in side[0] + vertical + side[1] + side[2]:
        message.start()
    known = along(infos.at[0])

    own_tl, own_bl = positive(to_left[...]), positive(-to_left[...])
    own_tr, own_br = positive(to_right[...]), positive(-to_right[...])
    for i, quarter in enumerate((own_tl, own_tr, own_bl, own_br)):
        recon[i] = tn(quarter, start[...])
    for message in vertical[:4]:
        message.arrived()
    up_bl, up_br = positive(from_up[...]), positive(-from_up[...])
    down_tl, down_tr = positive(from_down[...]), positive(-from_down[...])
    for i, (quarter, trace) in enumerate(
        ((up_bl, start_up), (up_br, start_up), (down_tl, start_down), (down_tr, start_down))
    ):
        recon[i] += tn(quarter, trace[...])
    for message in vertical[4:]:
        message.arrived()

    near_rows = (lax.broadcasted_iota(i32, (PIX, F), 0) & 31) < HALF

    def residual(pixels, near, i):
        seen = pixels[...].reshape(PIX, F).astype(f32)
        seen = jnp.where(near_rows, seen, 0.0) if near else jnp.where(near_rows, 0.0, seen)
        rest = seen - recon[i]
        high = rounded(rest)
        return jnp.concatenate([high, rest - high], axis=1).astype(bf16)

    rest_tl = residual(top_movie, True, 0)
    rest_tr = residual(top_movie, False, 1)
    rest_bl = residual(bottom_movie, True, 2)
    rest_br = residual(bottom_movie, False, 3)

    def halves(rows):
        l, r = from_left[rows, :], from_right[rows, :]
        return positive(l), positive(-l), positive(r), positive(-r)

    def side_sums(l_tr, l_br, r_tl, r_bl):
        l = nn(l_tr, rest_tl) + nn(l_br, rest_bl)
        r = nn(r_tl, rest_tr) + nn(r_bl, rest_br)
        return l[:, :F] + l[:, F:], r[:, :F] + r[:, F:]

    def side_parts(q):
        for message in side[q]:
            message.arrived()
        return halves(slice(q * ROWS, (q + 1) * ROWS))

    def to_band(l_tr, l_br, r_tl, r_bl):
        tl, bl, tr, br = (
            nn(jnp.concatenate([own[:ROWS], x], axis=0), rest)
            for own, x, rest in (
                (own_tl, l_tr, rest_tl), (own_bl, l_br, rest_bl),
                (own_tr, r_tl, rest_tr), (own_br, r_bl, rest_br),
            )
        )
        for i, x in enumerate(
            (tl[ROWS:] + bl[ROWS:], (tl + tr + bl + br)[:ROWS], tr[ROWS:] + br[ROWS:])
        ):
            about[i] = x[:, :F] + x[:, F:]
        messages = []
        for o in BAND:
            low, high = max(0, o[1]), min(3, 3 + o[1])
            messages.append(
                Remote(
                    about.at[pl.ds(low, high - low)],
                    abouts.at[1 - o[0], 2 - o[1], pl.ds(low - o[1], high - low)], o,
                ).start()
            )
        return messages

    def give_back(i, l_sum, r_sum):
        sum_left[i], sum_right[i] = l_sum, r_sum
        return [
            Remote(sum_left.at[i], sum_from_right.at[i], LEFT).start(),
            Remote(sum_right.at[i], sum_from_left.at[i], RIGHT).start(),
        ]

    def meet(q, l_tr, l_br, r_tl, r_bl):
        gram_tl, gram_bl = nt(l_tr, stack_tl), nt(l_br, stack_bl)
        gram_tr, gram_br = nt(r_tl, stack_tr), nt(r_bl, stack_br)
        cross_up[q] = jnp.concatenate([gram_tl[:, K:], gram_tr[:, K:]], axis=0)
        cross_down[q] = jnp.concatenate([gram_bl[:, K:], gram_br[:, K:]], axis=0)
        crossing = [
            Remote(cross_up.at[q], cross_from_down.at[q], UP).start(),
            Remote(cross_down.at[q], cross_from_up.at[q], DOWN).start(),
        ]
        return crossing, gram_tl[:, :K] + gram_bl[:, :K], gram_tr[:, :K] + gram_br[:, :K]

    met, returned = [], []
    for q in range(BLOCKS - 1):
        parts = side_parts(q)
        if q == 0:
            band = to_band(*parts)
            stack_tl = jnp.concatenate([own_tl, up_bl], axis=0)
            stack_tr = jnp.concatenate([own_tr, up_br], axis=0)
            stack_bl = jnp.concatenate([own_bl, down_tl], axis=0)
            stack_br = jnp.concatenate([own_br, down_tr], axis=0)
        else:
            returned.append(give_back(q - 1, *side_sums(*parts)))
        met.append(meet(q, *parts))
    for message in side[3]:
        message.start()
    known_late = along(infos.at[1])
    both = nn(own_tl, rest_tl) + nn(own_tr, rest_tr) + nn(own_bl, rest_bl) + nn(own_br, rest_br)
    total = both[:, :F] + both[:, F:]
    own_top = nt(stack_tl, own_tl) + nt(stack_tr, own_tr)
    own_bottom = nt(stack_bl, own_bl) + nt(stack_br, own_br)
    own_own = own_top[:K] + own_bottom[:K]
    own_up, own_down = own_top[K:], own_bottom[K:]

    def column(q):
        crossing, own_left, own_right = met[q]
        for message in crossing:
            message.arrived()
        mine = slice(q * ROWS, (q + 1) * ROWS)
        above, below = cross_from_up[q], cross_from_down[q]
        return jnp.concatenate(
            [above[:ROWS], own_up[mine], above[ROWS:], own_left, own_own[mine], own_right,
             below[:ROWS], own_down[mine], below[ROWS:]], axis=0
        ).T

    columns = [None] * (BLOCKS - 1)
    known = across(infos.at[0], known)
    columns[1] = column(1)
    margins[1, 1] = columns[1][2 * ROWS:3 * ROWS]
    lent = along(margins)
    columns[1] = lanes_of(columns[1])
    columns[0] = lanes_of(column(0))

    def stepped(previous, left_over, level):
        return jnp.maximum(previous + left_over / level, 0.0)

    def rows(q):
        return slice(q * ROWS, (q + 1) * ROWS)

    def facts(i, q):
        found = {HERE: (start_value[rows(q)], divisor[rows(q)])}
        for o in NEAR:
            if o != HERE:
                x = infos[i, o[0] + 1, o[1] + 1].astype(f32)
                level = x[ROWS:, 0:1] + x[ROWS:, 1:2] + x[ROWS:, 2:3]
                found[o] = (x[:ROWS], jnp.where(level == 0.0, 1.0, level))
        return found

    def band_sum(o):
        left_over = None
        for v in range(-2, 3):
            if abs(v - o[1]) > 1:
                continue
            piece = (
                about[o[1] + 1] if (o[0], v) == HERE
                else abouts[o[0] + 1, v + 2, o[1] + 1]
            )
            left_over = piece if left_over is None else left_over + piece
        return left_over

    for message in known:
        message.arrived()
    known_now = facts(0, 0)
    for message in band:
        message.arrived()
    moved = []
    for o in NEAR:
        previous, level = known_now[o]
        renewed = stepped(previous, band_sum(o), level)
        if o == HERE:
            renewed = jnp.where(alive_col[rows(0)], renewed, 0.0)
            current = [renewed]
        moved.append(renewed - previous)
    change = nn(columns[0][ROWS:], rows_of(jnp.concatenate(moved, axis=0)))

    for message in returned[0]:
        message.arrived()
    left_over = total[rows(1)] + sum_from_left[0] + sum_from_right[0] - change[:ROWS]
    previous = start_value[rows(1)]
    renewed = stepped(previous, left_over, divisor[rows(1)])
    renewed = jnp.where(alive_col[rows(1)], renewed, 0.0)
    current.append(renewed)
    own_step = renewed - previous
    step[...] = own_step
    moves = [
        Remote(
            step,
            steps.at[slot(flip(o))] if o in NEAR else far_steps.at[RING.index(flip(o))], o,
        ).start()
        for o in OUTWARD
    ]
    for message in returned[1]:
        message.arrived()
    own_sum = total[rows(2)] + sum_from_left[1] + sum_from_right[1] - change[ROWS:2 * ROWS]
    left_sum[...] = own_sum
    moves += [
        Remote(left_sum, left_sums.at[slot(flip(o))], o).start() for o in OUTWARD if o in NEAR
    ]
    returned_late = give_back(2, *side_sums(*side_parts(3)))
    known_late = across(infos.at[1], known_late)
    lent = across(margins, lent)
    columns[2] = lanes_of(column(2))
    for message in known_late:
        message.arrived()
    known_now = facts(1, 2)
    for message in lent:
        message.arrived()
    weights = {
        o: lanes_of(margins[o[0] + 1, o[1] + 1]) for o in NEAR
    }

    sent_last = moves + returned_late
    for message in sent:
        if message not in sent_last:
            message.left()
    for message in moves:
        message.arrived()
    taken = {
        o: own_step if o == HERE
        else steps[slot(o)] if o in NEAR
        else far_steps[RING.index(o)]
        for o in WIDE
    }
    moved = []
    for o in NEAR:
        nearby = rows_of(jnp.concatenate([taken[plus(o, p)] for p in NEAR], axis=0))
        if o == HERE:
            left_over = own_sum
            last_change = change[2 * ROWS:] + nn(columns[1][3 * ROWS:], nearby)
        else:
            left_over = left_sums[slot(o)]
        left_over = left_over - nn(weights[o], nearby)
        previous, level = known_now[o]
        renewed = stepped(previous, left_over, level)
        if o == HERE:
            renewed = jnp.where(alive_col[rows(2)], renewed, 0.0)
            current.append(renewed)
        moved.append(renewed - previous)

    last_change = last_change + nn(
        columns[2][3 * ROWS:], rows_of(jnp.concatenate(moved, axis=0))
    )
    for message in returned_late:
        message.arrived()
    last = total[rows(3)] + sum_from_left[2] + sum_from_right[2] - last_change
    renewed = stepped(start_value[rows(3)], last, divisor[rows(3)])
    current.append(jnp.where(alive_col[rows(3)], renewed, 0.0))
    result = jnp.concatenate(current, axis=0)
    high = rounded(result)
    mid = rounded(result - high)
    back = jnp.where(sub == order_row, 1.0, 0.0)
    out[...] = nn(
        jnp.concatenate([back, back, back], axis=1).astype(bf16),
        jnp.concatenate([high, mid, result - high - mid], axis=0).astype(bf16),
    )
    for message in sent_last:
        message.left()


def body(movie, footprints, centres, traces, counts, order):
    messages = 8 + 6 + 8 + len(BAND) + 6 + 6 + 4 + 32
    any_space = pl.BlockSpec(memory_space=pl.ANY)
    result = pl.pallas_call(
        kernel,
        name="hals",
        out_shape=pltpu.VMEM((K, F), f32),
        in_specs=[any_space] * 6,
        out_specs=pl.BlockSpec(memory_space=pltpu.VMEM),
        scratch_shapes=[
            pltpu.VMEM((K, PIX), bf16), pltpu.VMEM((2, K), i32), pltpu.VMEM((K, F), bf16),
            pltpu.VMEM((1, 1), i32), pltpu.VMEM((1, K), i32),
            pltpu.VMEM((SIDE, SIDE, F), bf16), pltpu.VMEM((SIDE, SIDE, F), bf16),
            *[pltpu.VMEM((K, PIX), bf16) for _ in range(8)],
            *[pltpu.VMEM((K, F), bf16) for _ in range(3)],
            pltpu.VMEM((2, 3, 3, 2 * ROWS, F), bf16),
            pltpu.VMEM((3, ROWS, F), f32), pltpu.VMEM((3, 5, 3, ROWS, F), f32),
            *[pltpu.VMEM((3, ROWS, F), f32) for _ in range(4)],
            *[pltpu.VMEM((3, 2 * ROWS, K), f32) for _ in range(4)],
            pltpu.VMEM((3, 3, ROWS, 9 * ROWS), f32),
            pltpu.VMEM((ROWS, F), f32), pltpu.VMEM((9, ROWS, F), f32),
            pltpu.VMEM((len(RING), ROWS, F), f32),
            pltpu.VMEM((ROWS, F), f32), pltpu.VMEM((9, ROWS, F), f32),
            pltpu.VMEM((4, PIX, F), f32),
            pltpu.SemaphoreType.DMA((7,)),
            pltpu.SemaphoreType.DMA((messages,)), pltpu.SemaphoreType.DMA((messages,)),
        ],
        compiler_params=pltpu.CompilerParams(collective_id=0, has_side_effects=True),
    )(movie, footprints[0, 0], centres[0, 0].T, traces[0, 0], counts, order[0])
    return result[None, None]


def solution(mesh):
    in_specs = (
        P("ty", "tx", None),
        P("ty", "tx", None, None),
        P("ty", "tx", None, None),
        P("ty", "tx", None, None),
        P("ty", "tx"),
        P("ty", "tx", None),
    )
    out_specs = P("ty", "tx", None, None)
    return jax.shard_map(body, mesh=mesh, in_specs=in_specs, out_specs=out_specs, check_vma=False)
```

```python
import jax
import jax.numpy as jnp
from jax import lax
from jax.experimental import pallas as pl
from jax.experimental.pallas import tpu as pltpu
from jax.sharding import PartitionSpec as P

K = 32
F = 128
SIDE = 32
PIX = SIDE * SIDE
HALF = SIDE // 2
ROWS = 8
BLOCKS = 4
MESH = pl.DeviceIdType.MESH
NEAR = [(u, v) for u in (-1, 0, 1) for v in (-1, 0, 1)]
WIDE = [(u, v) for u in range(-2, 3) for v in range(-2, 3)]
BAND = [(u, v) for u in (-1, 0, 1) for v in range(-2, 3) if (u, v) != (0, 0)]
HERE = (0, 0)
f32, bf16, i32 = jnp.float32, jnp.bfloat16, jnp.int32
UP, DOWN, LEFT, RIGHT = (-1, 0), (1, 0), (0, -1), (0, 1)


def flip(o):
    return (-o[0], -o[1])


def plus(o, p):
    return (o[0] + p[0], o[1] + p[1])


def nt(x, y):
    return lax.dot_general(x, y, (((1,), (1,)), ((), ())), preferred_element_type=f32)


def tn(x, y):
    return lax.dot_general(x, y, (((0,), (0,)), ((), ())), preferred_element_type=f32)


def nn(x, y):
    return jnp.dot(x, y, preferred_element_type=f32)


def rounded(x):
    return x.astype(bf16).astype(f32)


def lanes_of(x):
    high = rounded(x)
    return jnp.concatenate([high, high, x - high], axis=1).astype(bf16)


def rows_of(x):
    high = rounded(x)
    return jnp.concatenate([high, x - high, high], axis=0).astype(bf16)


def positive(x):
    return jnp.maximum(x, jnp.zeros_like(x))


def kernel(
    movie, foot_in, centres_in, traces_in, counts_in, order_in, out,
    foot, centres, traces, counts, order,
    top_movie, bottom_movie, to_left, to_right, to_up, to_down,
    from_right, from_left, from_down, from_up,
    start, start_up, start_down, infos,
    about, abouts, sum_left, sum_right, sum_from_right, sum_from_left,
    cross_up, cross_down, cross_from_down, cross_from_up,
    margins, step, steps, left_sum, left_sums, recon,
    local_sem, send_sem, recv_sem,
):
    a, b = lax.axis_index("ty"), lax.axis_index("tx")
    n_ty, n_tx = lax.axis_size("ty"), lax.axis_size("tx")

    def there(o):
        row, col = a + o[0], b + o[1]
        return (row >= 0) & (row < n_ty) & (col >= 0) & (col < n_tx)

    barrier = pltpu.get_barrier_semaphore()
    expected = jnp.int32(0)
    for o in NEAR:
        if o == HERE:
            continue
        present = there(o)

        @pl.when(present)
        def _(o=o):
            pl.semaphore_signal(
                barrier, inc=1, device_id=(a + o[0], b + o[1]), device_id_type=MESH
            )

        expected = expected + present.astype(i32)

    local = []
    for source, target in (
        (order_in, order), (counts_in, counts), (centres_in, centres), (foot_in, foot),
        (traces_in, traces), (movie.at[pl.ds(0, HALF)], top_movie.at[pl.ds(0, HALF)]),
        (movie.at[pl.ds(HALF, HALF)], bottom_movie.at[pl.ds(HALF, HALF)]),
    ):
        copy = pltpu.make_async_copy(source, target, local_sem.at[len(local)])
        copy.start()
        local.append(copy)

    sent = []

    class Remote:
        def __init__(self, source, target, o):
            self.o = o
            index = len(sent)
            self.copy = pltpu.make_async_remote_copy(
                src_ref=source, dst_ref=target,
                send_sem=send_sem.at[index], recv_sem=recv_sem.at[index],
                device_id=(a + o[0], b + o[1]), device_id_type=MESH,
            )
            sent.append(self)

        def start(self):
            pl.when(there(self.o))(self.copy.start)
            return self

        def arrived(self):
            pl.when(there(flip(self.o)))(self.copy.wait_recv)

        def left(self):
            pl.when(there(self.o))(self.copy.wait_send)

    class Fan:
        def __init__(self, source, place, reach, v):
            self.source, self.place, self.reach, self.v = source, place, reach, v
            self.index = len(sent)
            sent.append(self)

        def copy(self, source, target, u):
            return pltpu.make_async_remote_copy(
                src_ref=source, dst_ref=target,
                send_sem=send_sem.at[self.index], recv_sem=recv_sem.at[self.index],
                device_id=(a + u, b + self.v), device_id_type=MESH,
            )

        def start(self):
            for u in sorted(range(-self.reach, self.reach + 1), key=abs):
                copy = self.copy(self.source, self.place(self.reach - u), u)
                pl.when(there((u, self.v)))(copy.start)
            return self

        def wait(self, col, name):
            reach = self.reach
            rows = jnp.minimum(a, reach) + jnp.minimum(n_ty - 1 - a, reach) + 1
            for n in range(1, 2 * reach + 2):
                region = self.place(pl.ds(0, n))
                copy = self.copy(region, region, 0)
                pl.when((col >= 0) & (col < n_tx) & (rows == n))(getattr(copy, name))

        def arrived(self):
            self.wait(b - self.v, "wait_recv")

        def left(self):
            self.wait(b + self.v, "wait_send")

    def fan_out(source_of, place_of, reach, span):
        fans = [
            Fan(source_of(v), place_of(v), reach, v).start()
            for v in (-1, 1, -2, 2) if abs(v) <= span
        ]
        return fans + [
            Remote(source_of(0), place_of(0)(reach - u), (u, 0)).start()
            for u in (-1, 1, -2, 2) if abs(u) <= reach
        ]

    def clear(o, *refs):
        @pl.when(jnp.logical_not(there(o)))
        def _():
            for ref in refs:
                ref[...] = jnp.zeros_like(ref)

    clear(UP, from_up, start_up, cross_from_up, top_movie.at[pl.ds(HALF, HALF)])
    clear(DOWN, from_down, start_down, cross_from_down, bottom_movie.at[pl.ds(0, HALF)])
    clear(LEFT, from_left, sum_from_left)
    clear(RIGHT, from_right, sum_from_right)
    for o in NEAR:
        if o != HERE:
            clear(o, left_sums.at[o[1] + 1, o[0] + 1])
    for o in (UP, DOWN):
        clear(o, infos.at[0, o[0] + 1], infos.at[1, o[0] + 1], margins.at[o[0] + 1])
    for o in (LEFT, RIGHT):
        clear(o, infos.at[0, 1, o[1] + 1], infos.at[1, 1, o[1] + 1])
        clear(o, margins.at[1, o[1] + 1])
    for o in BAND:
        clear(o, abouts.at[o[1] + 2, o[0] + 1])
    for o in WIDE:
        if o != HERE:
            clear(o, steps.at[o[1] + 2, o[0] + 2])

    for copy in local[:3]:
        copy.wait()
    sub = lax.broadcasted_iota(i32, (K, K), 0)
    lane = lax.broadcasted_iota(i32, (K, K), 1)

    def to_column(row, pick):
        spread = jnp.where(pick, jnp.broadcast_to(row, (K, K)), 0)
        return jnp.sum(spread.astype(f32), axis=1, keepdims=True)

    order_row = order[0:1, :]
    order_col = to_column(order_row, sub == lane).astype(i32)
    alive_col = order_col < counts[0:1, 0:1]
    picked = (lane == order_col) & alive_col
    row_at = to_column(centres[0:1, :], picked).astype(i32)
    col_at = to_column(centres[1:2, :], picked).astype(i32)
    for copy in local[3:5]:
        copy.wait()
    chooser = jnp.where(picked, 1.0, 0.0).astype(bf16)
    ordered = nn(chooser, foot[...])
    start_value = nn(chooser, traces[...])
    start[...] = start_value.astype(bf16)
    diagonal = jnp.sum(ordered * ordered, axis=1, keepdims=True)
    divisor = jnp.where(alive_col, diagonal, 1.0)
    level = jnp.broadcast_to(divisor, (K, F))
    level_high = rounded(level)
    level_mid = rounded(level - level_high)
    level_low = level - level_high - level_mid
    wide_lane = lax.broadcasted_iota(i32, (K, F), 1)
    level_parts = jnp.where(
        wide_lane == 0, level_high, jnp.where(wide_lane == 1, level_mid, level_low)
    )
    for i, q in enumerate((0, 2)):
        infos[i, 1, 1] = jnp.concatenate(
            [x[q * ROWS:(q + 1) * ROWS] for x in (start_value, level_parts)], axis=0
        ).astype(bf16)

    group, across = wide_lane >> 5, wide_lane & 31
    turn, shift = (row_at + HALF) & 31, (col_at + HALF) & 31
    fine, coarse = turn & 3, turn >> 2
    index = (((group - fine) & 3) << 5) + ((across - shift) & 31)
    slabs = [
        jnp.take_along_axis(ordered[:, v * F:(v + 1) * F], index, axis=1) for v in range(8)
    ]
    carry = group < fine
    slabs = [jnp.where(carry, slabs[(v - 1) % 8], slabs[v]) for v in range(8)]
    for bit in (1, 2, 4):
        taken = jnp.broadcast_to((coarse & bit) != 0, (K, F))
        slabs = [jnp.where(taken, slabs[(v - bit) % 8], slabs[v]) for v in range(8)]
    left_half = ((across + HALF) & 31) >= col_at
    for v in range(8):
        upper = ((4 * v + group + HALF) & 31) >= row_at
        x = slabs[v]
        by_row = jnp.where(upper, x, -x)
        by_col = jnp.where(left_half, x, -x)
        here = pl.ds(v * F, F)
        to_left[:, here] = jnp.where(left_half, by_row, 0.0).astype(bf16)
        to_right[:, here] = jnp.where(left_half, 0.0, by_row).astype(bf16)
        to_up[:, here] = jnp.where(upper, by_col, 0.0).astype(bf16)
        to_down[:, here] = jnp.where(upper, 0.0, by_col).astype(bf16)
    for copy in local[5:]:
        copy.wait()

    pl.semaphore_wait(barrier, expected)

    def chunk(q):
        return pl.ds(q * ROWS, ROWS)

    side = [
        [Remote(to_left.at[chunk(q)], from_right.at[chunk(q)], LEFT),
         Remote(to_right.at[chunk(q)], from_left.at[chunk(q)], RIGHT)]
        for q in range(BLOCKS)
    ]
    vertical = [
        Remote(to_up, from_down, UP), Remote(to_down, from_up, DOWN),
        Remote(start, start_down, UP), Remote(start, start_up, DOWN),
        Remote(top_movie.at[pl.ds(0, HALF)], bottom_movie.at[pl.ds(0, HALF)], UP),
        Remote(bottom_movie.at[pl.ds(HALF, HALF)], top_movie.at[pl.ds(HALF, HALF)], DOWN),
    ]
    def along(ref):
        return [Remote(ref.at[1, 1], ref.at[1, 1 - o[1]], o).start() for o in (LEFT, RIGHT)]

    def across(ref, messages):
        for message in messages:
            message.arrived()
        return [Remote(ref.at[1], ref.at[1 - o[0]], o).start() for o in (UP, DOWN)]

    for message in side[0] + vertical + side[1] + side[2]:
        message.start()
    known = along(infos.at[0])

    own_tl, own_bl = positive(to_left[...]), positive(-to_left[...])
    own_tr, own_br = positive(to_right[...]), positive(-to_right[...])
    for i, quarter in enumerate((own_tl, own_tr, own_bl, own_br)):
        recon[i] = tn(quarter, start[...])
    for message in vertical[:4]:
        message.arrived()
    up_bl, up_br = positive(from_up[...]), positive(-from_up[...])
    down_tl, down_tr = positive(from_down[...]), positive(-from_down[...])
    for i, (quarter, trace) in enumerate(
        ((up_bl, start_up), (up_br, start_up), (down_tl, start_down), (down_tr, start_down))
    ):
        recon[i] += tn(quarter, trace[...])
    for message in vertical[4:]:
        message.arrived()

    near_rows = (lax.broadcasted_iota(i32, (PIX, F), 0) & 31) < HALF

    def residual(pixels, near, i):
        seen = pixels[...].reshape(PIX, F).astype(f32)
        seen = jnp.where(near_rows, seen, 0.0) if near else jnp.where(near_rows, 0.0, seen)
        rest = seen - recon[i]
        high = rounded(rest)
        return jnp.concatenate([high, rest - high], axis=1).astype(bf16)

    rest_tl = residual(top_movie, True, 0)
    rest_tr = residual(top_movie, False, 1)
    rest_bl = residual(bottom_movie, True, 2)
    rest_br = residual(bottom_movie, False, 3)

    def halves(rows):
        l, r = from_left[rows, :], from_right[rows, :]
        return positive(l), positive(-l), positive(r), positive(-r)

    def side_sums(l_tr, l_br, r_tl, r_bl):
        l = nn(l_tr, rest_tl) + nn(l_br, rest_bl)
        r = nn(r_tl, rest_tr) + nn(r_bl, rest_br)
        return l[:, :F] + l[:, F:], r[:, :F] + r[:, F:]

    def side_parts(q):
        for message in side[q]:
            message.arrived()
        return halves(slice(q * ROWS, (q + 1) * ROWS))

    def to_band(l_tr, l_br, r_tl, r_bl):
        tl, bl, tr, br = (
            nn(jnp.concatenate([own[:ROWS], x], axis=0), rest)
            for own, x, rest in (
                (own_tl, l_tr, rest_tl), (own_bl, l_br, rest_bl),
                (own_tr, r_tl, rest_tr), (own_br, r_bl, rest_br),
            )
        )
        for i, x in enumerate(
            (tl[ROWS:] + bl[ROWS:], (tl + tr + bl + br)[:ROWS], tr[ROWS:] + br[ROWS:])
        ):
            about[i] = x[:, :F] + x[:, F:]

        def piece(v):
            low, high = max(0, v), min(3, 3 + v)
            return about.at[pl.ds(low, high - low)]

        def place(v):
            low, high = max(0, v), min(3, 3 + v)
            return lambda rows: abouts.at[2 - v, rows, pl.ds(low - v, high - low)]

        return fan_out(piece, place, 1, 2)

    def give_back(i, l_sum, r_sum):
        sum_left[i], sum_right[i] = l_sum, r_sum
        return [
            Remote(sum_left.at[i], sum_from_right.at[i], LEFT).start(),
            Remote(sum_right.at[i], sum_from_left.at[i], RIGHT).start(),
        ]

    def meet(q, l_tr, l_br, r_tl, r_bl):
        gram_tl, gram_bl = nt(l_tr, stack_tl), nt(l_br, stack_bl)
        gram_tr, gram_br = nt(r_tl, stack_tr), nt(r_bl, stack_br)
        cross_up[q] = jnp.concatenate([gram_tl[:, K:], gram_tr[:, K:]], axis=0)
        cross_down[q] = jnp.concatenate([gram_bl[:, K:], gram_br[:, K:]], axis=0)
        crossing = [
            Remote(cross_up.at[q], cross_from_down.at[q], UP).start(),
            Remote(cross_down.at[q], cross_from_up.at[q], DOWN).start(),
        ]
        return crossing, gram_tl[:, :K] + gram_bl[:, :K], gram_tr[:, :K] + gram_br[:, :K]

    met, returned = [], []
    for q in range(BLOCKS - 1):
        parts = side_parts(q)
        if q == 0:
            band = to_band(*parts)
            stack_tl = jnp.concatenate([own_tl, up_bl], axis=0)
            stack_tr = jnp.concatenate([own_tr, up_br], axis=0)
            stack_bl = jnp.concatenate([own_bl, down_tl], axis=0)
            stack_br = jnp.concatenate([own_br, down_tr], axis=0)
        else:
            returned.append(give_back(q - 1, *side_sums(*parts)))
        met.append(meet(q, *parts))
    for message in side[3]:
        message.start()
    known_late = along(infos.at[1])
    both = nn(own_tl, rest_tl) + nn(own_tr, rest_tr) + nn(own_bl, rest_bl) + nn(own_br, rest_br)
    total = both[:, :F] + both[:, F:]
    own_top = nt(stack_tl, own_tl) + nt(stack_tr, own_tr)
    own_bottom = nt(stack_bl, own_bl) + nt(stack_br, own_br)
    own_own = own_top[:K] + own_bottom[:K]
    own_up, own_down = own_top[K:], own_bottom[K:]

    def column(q):
        crossing, own_left, own_right = met[q]
        for message in crossing:
            message.arrived()
        mine = slice(q * ROWS, (q + 1) * ROWS)
        above, below = cross_from_up[q], cross_from_down[q]
        return jnp.concatenate(
            [above[:ROWS], own_up[mine], above[ROWS:], own_left, own_own[mine], own_right,
             below[:ROWS], own_down[mine], below[ROWS:]], axis=0
        ).T

    columns = [None] * (BLOCKS - 1)
    known = across(infos.at[0], known)
    columns[1] = column(1)
    margins[1, 1] = columns[1][2 * ROWS:3 * ROWS]
    lent = along(margins)
    columns[1] = lanes_of(columns[1])
    columns[0] = lanes_of(column(0))

    def stepped(previous, left_over, level):
        return jnp.maximum(previous + left_over / level, 0.0)

    def rows(q):
        return slice(q * ROWS, (q + 1) * ROWS)

    def facts(i, q):
        found = {HERE: (start_value[rows(q)], divisor[rows(q)])}
        for o in NEAR:
            if o != HERE:
                x = infos[i, o[0] + 1, o[1] + 1].astype(f32)
                level = x[ROWS:, 0:1] + x[ROWS:, 1:2] + x[ROWS:, 2:3]
                found[o] = (x[:ROWS], jnp.where(level == 0.0, 1.0, level))
        return found

    def band_sum(o):
        left_over = None
        for v in range(-2, 3):
            if abs(v - o[1]) > 1:
                continue
            piece = (
                about[o[1] + 1] if (o[0], v) == HERE
                else abouts[v + 2, o[0] + 1, o[1] + 1]
            )
            left_over = piece if left_over is None else left_over + piece
        return left_over

    for message in known:
        message.arrived()
    known_now = facts(0, 0)
    for message in band:
        message.arrived()
    moved = []
    for o in NEAR:
        previous, level = known_now[o]
        renewed = stepped(previous, band_sum(o), level)
        if o == HERE:
            renewed = jnp.where(alive_col[rows(0)], renewed, 0.0)
            current = [renewed]
        moved.append(renewed - previous)
    change = nn(columns[0][ROWS:], rows_of(jnp.concatenate(moved, axis=0)))

    for message in returned[0]:
        message.arrived()
    left_over = total[rows(1)] + sum_from_left[0] + sum_from_right[0] - change[:ROWS]
    previous = start_value[rows(1)]
    renewed = stepped(previous, left_over, divisor[rows(1)])
    renewed = jnp.where(alive_col[rows(1)], renewed, 0.0)
    current.append(renewed)
    own_step = renewed - previous
    step[...] = own_step
    moves = fan_out(lambda v: step, lambda v: lambda rows: steps.at[2 - v, rows], 2, 2)
    for message in returned[1]:
        message.arrived()
    own_sum = total[rows(2)] + sum_from_left[1] + sum_from_right[1] - change[ROWS:2 * ROWS]
    left_sum[...] = own_sum
    moves += fan_out(
        lambda v: left_sum, lambda v: lambda rows: left_sums.at[1 - v, rows], 1, 1
    )
    returned_late = give_back(2, *side_sums(*side_parts(3)))
    known_late = across(infos.at[1], known_late)
    lent = across(margins, lent)
    columns[2] = lanes_of(column(2))
    for message in known_late:
        message.arrived()
    known_now = facts(1, 2)
    for message in lent:
        message.arrived()
    weights = {
        o: lanes_of(margins[o[0] + 1, o[1] + 1]) for o in NEAR
    }

    sent_last = moves + returned_late
    for message in sent:
        if message not in sent_last:
            message.left()
    for message in moves:
        message.arrived()
    taken = {
        o: own_step if o == HERE
        else steps[o[1] + 2, o[0] + 2]
        for o in WIDE
    }
    moved = []
    for o in NEAR:
        nearby = rows_of(jnp.concatenate([taken[plus(o, p)] for p in NEAR], axis=0))
        if o == HERE:
            left_over = own_sum
            last_change = change[2 * ROWS:] + nn(columns[1][3 * ROWS:], nearby)
        else:
            left_over = left_sums[o[1] + 1, o[0] + 1]
        left_over = left_over - nn(weights[o], nearby)
        previous, level = known_now[o]
        renewed = stepped(previous, left_over, level)
        if o == HERE:
            renewed = jnp.where(alive_col[rows(2)], renewed, 0.0)
            current.append(renewed)
        moved.append(renewed - previous)

    last_change = last_change + nn(
        columns[2][3 * ROWS:], rows_of(jnp.concatenate(moved, axis=0))
    )
    for message in returned_late:
        message.arrived()
    last = total[rows(3)] + sum_from_left[2] + sum_from_right[2] - last_change
    renewed = stepped(start_value[rows(3)], last, divisor[rows(3)])
    current.append(jnp.where(alive_col[rows(3)], renewed, 0.0))
    result = jnp.concatenate(current, axis=0)
    high = rounded(result)
    mid = rounded(result - high)
    back = jnp.where(sub == order_row, 1.0, 0.0)
    out[...] = nn(
        jnp.concatenate([back, back, back], axis=1).astype(bf16),
        jnp.concatenate([high, mid, result - high - mid], axis=0).astype(bf16),
    )
    for message in sent_last:
        message.left()


def body(movie, footprints, centres, traces, counts, order):
    messages = 8 + 6 + 8 + 6 + 6 + 6 + 4 + 8 + 4
    any_space = pl.BlockSpec(memory_space=pl.ANY)
    result = pl.pallas_call(
        kernel,
        name="hals",
        out_shape=pltpu.VMEM((K, F), f32),
        in_specs=[any_space] * 6,
        out_specs=pl.BlockSpec(memory_space=pltpu.VMEM),
        scratch_shapes=[
            pltpu.VMEM((K, PIX), bf16), pltpu.VMEM((2, K), i32), pltpu.VMEM((K, F), bf16),
            pltpu.VMEM((1, 1), i32), pltpu.VMEM((1, K), i32),
            pltpu.VMEM((SIDE, SIDE, F), bf16), pltpu.VMEM((SIDE, SIDE, F), bf16),
            *[pltpu.VMEM((K, PIX), bf16) for _ in range(8)],
            *[pltpu.VMEM((K, F), bf16) for _ in range(3)],
            pltpu.VMEM((2, 3, 3, 2 * ROWS, F), bf16),
            pltpu.VMEM((3, ROWS, F), f32), pltpu.VMEM((5, 3, 3, ROWS, F), f32),
            *[pltpu.VMEM((3, ROWS, F), f32) for _ in range(4)],
            *[pltpu.VMEM((3, 2 * ROWS, K), f32) for _ in range(4)],
            pltpu.VMEM((3, 3, ROWS, 9 * ROWS), f32),
            pltpu.VMEM((ROWS, F), f32), pltpu.VMEM((5, 5, ROWS, F), f32),
            pltpu.VMEM((ROWS, F), f32), pltpu.VMEM((3, 3, ROWS, F), f32),
            pltpu.VMEM((4, PIX, F), f32),
            pltpu.SemaphoreType.DMA((7,)),
            pltpu.SemaphoreType.DMA((messages,)), pltpu.SemaphoreType.DMA((messages,)),
        ],
        compiler_params=pltpu.CompilerParams(collective_id=0, has_side_effects=True),
    )(movie, footprints[0, 0], centres[0, 0].T, traces[0, 0], counts, order[0])
    return result[None, None]


def solution(mesh):
    in_specs = (
        P("ty", "tx", None),
        P("ty", "tx", None, None),
        P("ty", "tx", None, None),
        P("ty", "tx", None, None),
        P("ty", "tx"),
        P("ty", "tx", None),
    )
    out_specs = P("ty", "tx", None, None)
    return jax.shard_map(body, mesh=mesh, in_specs=in_specs, out_specs=out_specs, check_vma=False)
```

```python
import jax
import jax.numpy as jnp
from jax import lax
from jax.experimental import pallas as pl
from jax.experimental.pallas import tpu as pltpu
from jax.sharding import PartitionSpec as P

K = 32
F = 128
SIDE = 32
PIX = SIDE * SIDE
HALF = SIDE // 2
ROWS = 8
BLOCKS = 4
MESH = pl.DeviceIdType.MESH
NEAR = [(u, v) for u in (-1, 0, 1) for v in (-1, 0, 1)]
WIDE = [(u, v) for u in range(-2, 3) for v in range(-2, 3)]
BAND = [(u, v) for u in (-1, 0, 1) for v in range(-2, 3) if (u, v) != (0, 0)]
HERE = (0, 0)
f32, bf16, i32 = jnp.float32, jnp.bfloat16, jnp.int32
UP, DOWN, LEFT, RIGHT = (-1, 0), (1, 0), (0, -1), (0, 1)


def flip(o):
    return (-o[0], -o[1])


def plus(o, p):
    return (o[0] + p[0], o[1] + p[1])


def nt(x, y):
    return lax.dot_general(x, y, (((1,), (1,)), ((), ())), preferred_element_type=f32)


def tn(x, y):
    return lax.dot_general(x, y, (((0,), (0,)), ((), ())), preferred_element_type=f32)


def nn(x, y):
    return jnp.dot(x, y, preferred_element_type=f32)


def rounded(x):
    return x.astype(bf16).astype(f32)


def lanes_of(x):
    high = rounded(x)
    return jnp.concatenate([high, high, x - high], axis=1).astype(bf16)


def rows_of(x):
    high = rounded(x)
    return jnp.concatenate([high, x - high, high], axis=0).astype(bf16)


def positive(x):
    return jnp.maximum(x, jnp.zeros_like(x))


def kernel(
    movie, foot_in, centres_in, traces_in, counts_in, order_in, out,
    foot, centres, traces, counts, order,
    top_movie, bottom_movie, to_left, to_right, to_up, to_down,
    from_right, from_left, from_down, from_up,
    start, start_up, start_down, infos,
    about, abouts, sum_left, sum_right, sum_from_right, sum_from_left,
    cross_up, cross_down, cross_from_down, cross_from_up,
    margins, step, steps, left_sum, left_sums, recon,
    local_sem, send_sem, recv_sem,
):
    a, b = lax.axis_index("ty"), lax.axis_index("tx")
    n_ty, n_tx = lax.axis_size("ty"), lax.axis_size("tx")
    odd = lax.rem(b, 2) == 1

    def there(o):
        row, col = a + o[0], b + o[1]
        return (row >= 0) & (row < n_ty) & (col >= 0) & (col < n_tx)

    barrier = pltpu.get_barrier_semaphore()
    expected = jnp.int32(0)
    for o in NEAR:
        if o == HERE:
            continue
        present = there(o)

        @pl.when(present)
        def _(o=o):
            pl.semaphore_signal(
                barrier, inc=1, device_id=(a + o[0], b + o[1]), device_id_type=MESH
            )

        expected = expected + present.astype(i32)

    local = []
    for source, target in (
        (order_in, order), (counts_in, counts), (centres_in, centres), (foot_in, foot),
        (traces_in, traces), (movie.at[pl.ds(0, HALF)], top_movie.at[pl.ds(0, HALF)]),
        (movie.at[pl.ds(HALF, HALF)], bottom_movie.at[pl.ds(HALF, HALF)]),
    ):
        copy = pltpu.make_async_copy(source, target, local_sem.at[len(local)])
        copy.start()
        local.append(copy)

    sent = []

    class Group:
        def __init__(self, messages, region):
            self.messages, self.region = messages, region
            self.index = len(sent)
            sent.append(self)

        def copy(self, source, target, o):
            return pltpu.make_async_remote_copy(
                src_ref=source, dst_ref=target,
                send_sem=send_sem.at[self.index], recv_sem=recv_sem.at[self.index],
                device_id=(a + o[0], b + o[1]), device_id_type=MESH,
            )

        def start(self):
            begin = [
                (there(o), self.copy(source, target, o), o) for source, target, o in self.messages
            ]
            for present, copy, o in begin:
                if o == RIGHT:
                    pl.when(present & odd)(copy.start)
            for present, copy, o in begin:
                if o != RIGHT:
                    pl.when(present)(copy.start)
            for present, copy, o in begin:
                if o == RIGHT:
                    pl.when(present & jnp.logical_not(odd))(copy.start)
            return self

        def wait(self, name):
            present = sum(there(o).astype(i32) for _, _, o in self.messages)
            for n in range(1, len(self.messages) + 1):
                region = self.region(n)
                copy = self.copy(region, region, self.messages[0][2])
                pl.when(present == n)(getattr(copy, name))

        def arrived(self):
            self.wait("wait_recv")

        def left(self):
            self.wait("wait_send")

    class Fan:
        def __init__(self, source, place, reach, v):
            self.source, self.place, self.reach, self.v = source, place, reach, v
            self.index = len(sent)
            sent.append(self)

        def copy(self, source, target, u):
            return pltpu.make_async_remote_copy(
                src_ref=source, dst_ref=target,
                send_sem=send_sem.at[self.index], recv_sem=recv_sem.at[self.index],
                device_id=(a + u, b + self.v), device_id_type=MESH,
            )

        def start(self, turn=None):
            for u in sorted(range(-self.reach, self.reach + 1), key=abs):
                copy = self.copy(self.source, self.place(self.reach - u), u)
                present = there((u, self.v))
                pl.when(present if turn is None else present & turn)(copy.start)
            return self

        def wait(self, col, name):
            reach = self.reach
            rows = jnp.minimum(a, reach) + jnp.minimum(n_ty - 1 - a, reach) + 1
            for n in range(1, 2 * reach + 2):
                region = self.place(pl.ds(0, n))
                copy = self.copy(region, region, 0)
                pl.when((col >= 0) & (col < n_tx) & (rows == n))(getattr(copy, name))

        def arrived(self):
            self.wait(b - self.v, "wait_recv")

        def left(self):
            self.wait(b + self.v, "wait_send")

    def fan_out(source_of, place_of, reach, span):
        fans = [
            Fan(source_of(v), place_of(v), reach, v) for v in (-1, 1, -2, 2) if abs(v) <= span
        ]
        fans[1].start(odd)
        fans[0].start()
        fans[1].start(jnp.logical_not(odd))
        for fan in fans[2:]:
            fan.start()
        own = [
            (source_of(0), place_of(0)(reach - u), (u, 0))
            for u in (-1, 1, -2, 2) if abs(u) <= reach
        ]
        return fans + [Group(own, lambda n: place_of(0)(pl.ds(0, n))).start()]

    def clear(o, *refs):
        @pl.when(jnp.logical_not(there(o)))
        def _():
            for ref in refs:
                ref[...] = jnp.zeros_like(ref)

    clear(UP, from_up, start_up, cross_from_up, top_movie.at[pl.ds(HALF, HALF)])
    clear(DOWN, from_down, start_down, cross_from_down, bottom_movie.at[pl.ds(0, HALF)])
    clear(LEFT, from_left, sum_from_left)
    clear(RIGHT, from_right, sum_from_right)
    for o in NEAR:
        if o != HERE:
            clear(o, left_sums.at[o[1] + 1, o[0] + 1])
            clear(o, margins.at[o[1] + 1, o[0] + 1])
    for o in (UP, DOWN):
        clear(o, infos.at[o[0] + 1])
    for o in (LEFT, RIGHT):
        clear(o, infos.at[1, o[1] + 1])
    for o in BAND:
        clear(o, abouts.at[o[1] + 2, o[0] + 1])
    for o in WIDE:
        if o != HERE:
            clear(o, steps.at[o[1] + 2, o[0] + 2])

    for copy in local[:3]:
        copy.wait()
    sub = lax.broadcasted_iota(i32, (K, K), 0)
    lane = lax.broadcasted_iota(i32, (K, K), 1)

    def to_column(row, pick):
        spread = jnp.where(pick, jnp.broadcast_to(row, (K, K)), 0)
        return jnp.sum(spread.astype(f32), axis=1, keepdims=True)

    order_row = order[0:1, :]
    order_col = to_column(order_row, sub == lane).astype(i32)
    alive_col = order_col < counts[0:1, 0:1]
    picked = (lane == order_col) & alive_col
    row_at = to_column(centres[0:1, :], picked).astype(i32)
    col_at = to_column(centres[1:2, :], picked).astype(i32)
    for copy in local[3:5]:
        copy.wait()
    chooser = jnp.where(picked, 1.0, 0.0).astype(bf16)
    ordered = nn(chooser, foot[...])
    start_value = nn(chooser, traces[...])
    start[...] = start_value.astype(bf16)
    diagonal = jnp.sum(ordered * ordered, axis=1, keepdims=True)
    divisor = jnp.where(alive_col, diagonal, 1.0)
    level = jnp.broadcast_to(divisor, (K, F))
    level_high = rounded(level)
    level_mid = rounded(level - level_high)
    level_low = level - level_high - level_mid
    wide_lane = lax.broadcasted_iota(i32, (K, F), 1)
    level_parts = jnp.where(
        wide_lane == 0, level_high, jnp.where(wide_lane == 1, level_mid, level_low)
    )
    for i, q in enumerate((0, 2)):
        infos[1, 1, i] = jnp.concatenate(
            [x[q * ROWS:(q + 1) * ROWS] for x in (start_value, level_parts)], axis=0
        ).astype(bf16)

    group, across = wide_lane >> 5, wide_lane & 31
    turn, shift = (row_at + HALF) & 31, (col_at + HALF) & 31
    fine, coarse = turn & 3, turn >> 2
    index = (((group - fine) & 3) << 5) + ((across - shift) & 31)
    slabs = [
        jnp.take_along_axis(ordered[:, v * F:(v + 1) * F], index, axis=1) for v in range(8)
    ]
    carry = group < fine
    slabs = [jnp.where(carry, slabs[(v - 1) % 8], slabs[v]) for v in range(8)]
    for bit in (1, 2, 4):
        taken = jnp.broadcast_to((coarse & bit) != 0, (K, F))
        slabs = [jnp.where(taken, slabs[(v - bit) % 8], slabs[v]) for v in range(8)]
    left_half = ((across + HALF) & 31) >= col_at
    for v in range(8):
        upper = ((4 * v + group + HALF) & 31) >= row_at
        x = slabs[v]
        by_row = jnp.where(upper, x, -x)
        by_col = jnp.where(left_half, x, -x)
        here = pl.ds(v * F, F)
        to_left[:, here] = jnp.where(left_half, by_row, 0.0).astype(bf16)
        to_right[:, here] = jnp.where(left_half, 0.0, by_row).astype(bf16)
        to_up[:, here] = jnp.where(upper, by_col, 0.0).astype(bf16)
        to_down[:, here] = jnp.where(upper, 0.0, by_col).astype(bf16)
    for copy in local[5:]:
        copy.wait()

    pl.semaphore_wait(barrier, expected)

    def chunk(q):
        return pl.ds(q * ROWS, ROWS)

    side = [
        [Group(
            [(to_left.at[chunk(q)], from_right.at[chunk(q)], LEFT),
             (to_right.at[chunk(q)], from_left.at[chunk(q)], RIGHT)],
            lambda n: from_left.at[pl.ds(0, n * ROWS)],
        )]
        for q in range(BLOCKS)
    ]
    first_rows, last_rows = pl.ds(0, HALF), pl.ds(HALF, HALF)
    vertical = [
        Group(
            [(to_up, from_down, UP), (to_down, from_up, DOWN)],
            lambda n: top_movie.at[pl.ds(0, n * HALF // 2)],
        ),
        Group(
            [(start, start_down, UP), (start, start_up, DOWN)],
            lambda n: from_up.at[pl.ds(0, n * ROWS // 2)] if n == 2 else start_up,
        ),
        Group(
            [(top_movie.at[first_rows], bottom_movie.at[first_rows], UP),
             (bottom_movie.at[last_rows], top_movie.at[last_rows], DOWN)],
            lambda n: top_movie.at[pl.ds(0, n * HALF)],
        ),
    ]

    def along(ref):
        messages = [(ref.at[1, 1], ref.at[1, 1 - o[1]], o) for o in (LEFT, RIGHT)]
        return [Group(messages, lambda n: ref.at[0, pl.ds(0, n)]).start()]

    def across(ref, messages):
        for message in messages:
            message.arrived()
        messages = [(ref.at[1], ref.at[1 - o[0]], o) for o in (UP, DOWN)]
        return [Group(messages, lambda n: ref.at[pl.ds(0, n)]).start()]

    for message in side[0] + vertical + side[1]:
        message.start()
    known = along(infos)
    for message in side[2]:
        message.start()

    own_tl, own_bl = positive(to_left[...]), positive(-to_left[...])
    own_tr, own_br = positive(to_right[...]), positive(-to_right[...])
    for i, quarter in enumerate((own_tl, own_tr, own_bl, own_br)):
        recon[i] = tn(quarter, start[...])
    for message in vertical[:2]:
        message.arrived()
    up_bl, up_br = positive(from_up[...]), positive(-from_up[...])
    down_tl, down_tr = positive(from_down[...]), positive(-from_down[...])
    def seen(i, quarter, trace):
        whole = recon[i] + tn(quarter, trace[...])
        high = rounded(whole)
        return jnp.concatenate([high, whole - high], axis=1).astype(bf16)

    seen_tl, seen_tr = seen(0, up_bl, start_up), seen(1, up_br, start_up)
    seen_bl, seen_br = seen(2, down_tl, start_down), seen(3, down_tr, start_down)

    def folded(x):
        return x[:, :F] + x[:, F:]

    own_seen = folded(
        nn(own_tl, seen_tl) + nn(own_tr, seen_tr) + nn(own_bl, seen_bl) + nn(own_br, seen_br)
    )
    near_side = (lax.broadcasted_iota(i32, (K, PIX), 1) & 31) < HALF
    near_side = jnp.where(near_side, 1.0, 0.0).astype(bf16)
    far_side = 1.0 - near_side
    strip_top = own_tl * near_side + own_tr * far_side
    strip_bottom = own_bl * near_side + own_br * far_side

    def halves(rows):
        l, r = from_left[rows, :], from_right[rows, :]
        return positive(l), positive(-l), positive(r), positive(-r)

    def side_seen(l_tr, l_br, r_tl, r_bl):
        l = folded(nn(l_tr, seen_tl) + nn(l_br, seen_bl))
        r = folded(nn(r_tl, seen_tr) + nn(r_bl, seen_br))
        return l, r

    def driven(upper, lower):
        above, below = (x[...].reshape(PIX, F) for x in (top_movie, bottom_movie))
        return nn(jnp.concatenate(upper, axis=0), above) + nn(jnp.concatenate(lower, axis=0), below)

    def strips(l_tr, l_br, r_tl, r_bl):
        near, far = near_side[:ROWS], far_side[:ROWS]
        return [l_tr * near, r_tl * far], [l_br * near, r_bl * far]

    def side_sums(*parts):
        l, r = side_seen(*parts)
        both = driven(*strips(*parts))
        return both[:ROWS] - l, both[ROWS:] - r

    def side_parts(q):
        for message in side[q]:
            message.arrived()
        return halves(slice(q * ROWS, (q + 1) * ROWS))

    def to_band(l_tr, l_br, r_tl, r_bl):
        l, r = side_seen(l_tr, l_br, r_tl, r_bl)
        upper, lower = strips(l_tr, l_br, r_tl, r_bl)
        for message in vertical[2:]:
            message.arrived()
        three = driven([strip_top[:ROWS]] + upper, [strip_bottom[:ROWS]] + lower)
        about[0] = three[ROWS:2 * ROWS] - l
        about[1] = three[:ROWS] - own_seen[:ROWS]
        about[2] = three[2 * ROWS:] - r

        def piece(v):
            low, high = max(0, v), min(3, 3 + v)
            return about.at[pl.ds(low, high - low)]

        def place(v):
            low, high = max(0, v), min(3, 3 + v)
            return lambda rows: abouts.at[2 - v, rows, pl.ds(low - v, high - low)]

        return fan_out(piece, place, 1, 2)

    def give_back(i, l_sum, r_sum):
        sum_left[i], sum_right[i] = l_sum, r_sum
        messages = [
            (sum_left.at[i], sum_from_right.at[i], LEFT),
            (sum_right.at[i], sum_from_left.at[i], RIGHT),
        ]
        return [Group(messages, lambda n: sum_from_left.at[pl.ds(0, n)]).start()]

    def meet(q, l_tr, l_br, r_tl, r_bl):
        gram_tl, gram_bl = nt(l_tr, stack_tl), nt(l_br, stack_bl)
        gram_tr, gram_br = nt(r_tl, stack_tr), nt(r_bl, stack_br)
        cross_up[q] = jnp.concatenate([gram_tl[:, K:], gram_tr[:, K:]], axis=0)
        cross_down[q] = jnp.concatenate([gram_bl[:, K:], gram_br[:, K:]], axis=0)
        messages = [
            (cross_up.at[q], cross_from_down.at[q], UP),
            (cross_down.at[q], cross_from_up.at[q], DOWN),
        ]
        crossing = [Group(messages, lambda n: cross_from_up.at[pl.ds(0, n)]).start()]
        return crossing, gram_tl[:, :K] + gram_bl[:, :K], gram_tr[:, :K] + gram_br[:, :K]

    met, returned = [], []
    for q in range(BLOCKS - 1):
        if q == 2:
            known = across(infos, known)
        parts = side_parts(q)
        if q == 0:
            band = to_band(*parts)
            stack_tl = jnp.concatenate([own_tl, up_bl], axis=0)
            stack_tr = jnp.concatenate([own_tr, up_br], axis=0)
            stack_bl = jnp.concatenate([own_bl, down_tl], axis=0)
            stack_br = jnp.concatenate([own_br, down_tr], axis=0)
        else:
            returned.append(give_back(q - 1, *side_sums(*parts)))
        met.append(meet(q, *parts))
    for message in side[3]:
        message.start()
    total = driven([strip_top], [strip_bottom]) - own_seen
    own_top = nt(stack_tl, own_tl) + nt(stack_tr, own_tr)
    own_bottom = nt(stack_bl, own_bl) + nt(stack_br, own_br)
    own_own = own_top[:K] + own_bottom[:K]
    own_up, own_down = own_top[K:], own_bottom[K:]

    def column(q):
        crossing, own_left, own_right = met[q]
        for message in crossing:
            message.arrived()
        mine = slice(q * ROWS, (q + 1) * ROWS)
        above, below = cross_from_up[q], cross_from_down[q]
        return jnp.concatenate(
            [above[:ROWS], own_up[mine], above[ROWS:], own_left, own_own[mine], own_right,
             below[:ROWS], own_down[mine], below[ROWS:]], axis=0
        ).T

    columns = [None] * (BLOCKS - 1)
    columns[1] = column(1)
    margins[1, 1] = columns[1][2 * ROWS:3 * ROWS]
    lent = fan_out(
        lambda v: margins.at[1, 1], lambda v: lambda rows: margins.at[1 - v, rows], 1, 1
    )
    columns[1] = lanes_of(columns[1])
    columns[0] = lanes_of(column(0))

    def stepped(previous, left_over, level):
        return jnp.maximum(previous + left_over / level, 0.0)

    def rows(q):
        return slice(q * ROWS, (q + 1) * ROWS)

    def facts(i, q):
        found = {HERE: (start_value[rows(q)], divisor[rows(q)])}
        for o in NEAR:
            if o != HERE:
                x = infos[o[0] + 1, o[1] + 1, i].astype(f32)
                level = x[ROWS:, 0:1] + x[ROWS:, 1:2] + x[ROWS:, 2:3]
                found[o] = (x[:ROWS], jnp.where(level == 0.0, 1.0, level))
        return found

    def band_sum(o):
        left_over = None
        for v in range(-2, 3):
            if abs(v - o[1]) > 1:
                continue
            piece = (
                about[o[1] + 1] if (o[0], v) == HERE
                else abouts[v + 2, o[0] + 1, o[1] + 1]
            )
            left_over = piece if left_over is None else left_over + piece
        return left_over

    for message in known:
        message.arrived()
    known_now = facts(0, 0)
    for message in band:
        message.arrived()
    moved = []
    for o in NEAR:
        previous, level = known_now[o]
        renewed = stepped(previous, band_sum(o), level)
        if o == HERE:
            renewed = jnp.where(alive_col[rows(0)], renewed, 0.0)
            current = [renewed]
        moved.append(renewed - previous)
    change = nn(columns[0][ROWS:], rows_of(jnp.concatenate(moved, axis=0)))

    for message in returned[0]:
        message.arrived()
    left_over = total[rows(1)] + sum_from_left[0] + sum_from_right[0] - change[:ROWS]
    previous = start_value[rows(1)]
    renewed = stepped(previous, left_over, divisor[rows(1)])
    renewed = jnp.where(alive_col[rows(1)], renewed, 0.0)
    current.append(renewed)
    own_step = renewed - previous
    step[...] = own_step
    moves = fan_out(lambda v: step, lambda v: lambda rows: steps.at[2 - v, rows], 2, 2)
    for message in returned[1]:
        message.arrived()
    own_sum = total[rows(2)] + sum_from_left[1] + sum_from_right[1] - change[ROWS:2 * ROWS]
    left_sum[...] = own_sum
    moves += fan_out(
        lambda v: left_sum, lambda v: lambda rows: left_sums.at[1 - v, rows], 1, 1
    )
    returned_late = give_back(2, *side_sums(*side_parts(3)))
    columns[2] = lanes_of(column(2))
    known_now = facts(1, 2)
    for message in lent:
        message.arrived()
    weights = {
        o: lanes_of(margins[o[1] + 1, o[0] + 1]) for o in NEAR
    }

    sent_last = moves + returned_late
    for message in sent:
        if message not in sent_last:
            message.left()
    for message in moves:
        message.arrived()
    taken = {
        o: own_step if o == HERE
        else steps[o[1] + 2, o[0] + 2]
        for o in WIDE
    }
    moved = []
    for o in NEAR:
        nearby = rows_of(jnp.concatenate([taken[plus(o, p)] for p in NEAR], axis=0))
        if o == HERE:
            left_over = own_sum
            last_change = change[2 * ROWS:] + nn(columns[1][3 * ROWS:], nearby)
        else:
            left_over = left_sums[o[1] + 1, o[0] + 1]
        left_over = left_over - nn(weights[o], nearby)
        previous, level = known_now[o]
        renewed = stepped(previous, left_over, level)
        if o == HERE:
            renewed = jnp.where(alive_col[rows(2)], renewed, 0.0)
            current.append(renewed)
        moved.append(renewed - previous)

    last_change = last_change + nn(
        columns[2][3 * ROWS:], rows_of(jnp.concatenate(moved, axis=0))
    )
    for message in returned_late:
        message.arrived()
    last = total[rows(3)] + sum_from_left[2] + sum_from_right[2] - last_change
    renewed = stepped(start_value[rows(3)], last, divisor[rows(3)])
    current.append(jnp.where(alive_col[rows(3)], renewed, 0.0))
    result = jnp.concatenate(current, axis=0)
    high = rounded(result)
    mid = rounded(result - high)
    back = jnp.where(sub == order_row, 1.0, 0.0)
    out[...] = nn(
        jnp.concatenate([back, back, back], axis=1).astype(bf16),
        jnp.concatenate([high, mid, result - high - mid], axis=0).astype(bf16),
    )
    for message in sent_last:
        message.left()


def body(movie, footprints, centres, traces, counts, order):
    messages = 4 + 3 + 2 + 5 + 3 + 3 + 3 + 5 + 3
    any_space = pl.BlockSpec(memory_space=pl.ANY)
    result = pl.pallas_call(
        kernel,
        name="hals",
        out_shape=pltpu.VMEM((K, F), f32),
        in_specs=[any_space] * 6,
        out_specs=pl.BlockSpec(memory_space=pltpu.VMEM),
        scratch_shapes=[
            pltpu.VMEM((K, PIX), bf16), pltpu.VMEM((2, K), i32), pltpu.VMEM((K, F), bf16),
            pltpu.VMEM((1, 1), i32), pltpu.VMEM((1, K), i32),
            pltpu.VMEM((SIDE, SIDE, F), bf16), pltpu.VMEM((SIDE, SIDE, F), bf16),
            *[pltpu.VMEM((K, PIX), bf16) for _ in range(8)],
            *[pltpu.VMEM((K, F), bf16) for _ in range(3)],
            pltpu.VMEM((3, 3, 2, 2 * ROWS, F), bf16),
            pltpu.VMEM((3, ROWS, F), f32), pltpu.VMEM((5, 3, 3, ROWS, F), f32),
            *[pltpu.VMEM((3, ROWS, F), f32) for _ in range(4)],
            *[pltpu.VMEM((3, 2 * ROWS, K), f32) for _ in range(4)],
            pltpu.VMEM((3, 3, ROWS, 9 * ROWS), f32),
            pltpu.VMEM((ROWS, F), f32), pltpu.VMEM((5, 5, ROWS, F), f32),
            pltpu.VMEM((ROWS, F), f32), pltpu.VMEM((3, 3, ROWS, F), f32),
            pltpu.VMEM((4, PIX, F), f32),
            pltpu.SemaphoreType.DMA((7,)),
            pltpu.SemaphoreType.DMA((messages,)), pltpu.SemaphoreType.DMA((messages,)),
        ],
        compiler_params=pltpu.CompilerParams(
            collective_id=0, has_side_effects=True
        ),
    )(movie, footprints[0, 0], centres[0, 0].T, traces[0, 0], counts, order[0])
    return result[None, None]


def solution(mesh):
    in_specs = (
        P("ty", "tx", None),
        P("ty", "tx", None, None),
        P("ty", "tx", None, None),
        P("ty", "tx", None, None),
        P("ty", "tx"),
        P("ty", "tx", None),
    )
    out_specs = P("ty", "tx", None, None)
    return jax.shard_map(body, mesh=mesh, in_specs=in_specs, out_specs=out_specs, check_vma=False)
```
